32 devices in a mesh: row: 4 (over y, x), col: 8 (over z, core).
Axes of the slice: x: 2, y: 2, z: 4, core: 2. Of those that a mesh axis runs over, the one named last changes fastest.
Arguments:
- boxes: int32 [4, 16384], P(None, 'col'), may hold values from 0 to 2047, as said below
- pins: int32 [16384], P('col'), may hold values from 2 to 64
- capacity: float32 [2048, 1024], P('row', 'col'), may hold values from 4 to 12
- cell_bin: int32 [4, 16384], P('row', 'col'), may hold values from 0 to 65535
- cell_area: float32 [4, 16384], P('row', 'col'), may hold values from 1 to 10
Outputs:
- rudy: float32 [2048, 1024], P('row', 'col')
- inflation: float32 [2048, 1024], P('row', 'col')
- cell_sizes: float32 [4, 16384], P('row', 'col')
The draws below stay inside these ranges and needn't reach their ends.
Inputs may be any that keep to these rules, and one draw needn't show every extreme that they name: `boxes`: row 0 and 1 are a net's first and last bin column, row 2 and 3 its first and last bin row; first <= last, a box spans at most 128 columns and 256 rows.
All inputs are finite; a program needn't handle non-finite values.
Results may differ from the reference program's by a relative error of at most 0.0003.
Values sent between devices are 32-bit elements; how exact they have to be, the bound alone decides.
A program may use at most 64 MiB of HBM per device.

```python
import math
import jax
import jax.numpy as jnp

TILE_R = 512
TILE_C = 128
CELLS_DEV = 2048
GY = 2048
GX = 1024
NETS = 16384
SPAN_X = 128
SPAN_Y = 256
N_ROW = 4
N_COL = 8


def draw_boxes(key, part):
    keys = jax.random.split(key, 4)
    start_x = jax.random.randint(keys[0], (NETS,), 0, GX)
    width_x = jax.random.randint(keys[1], (NETS,), 1, SPAN_X + 1)
    start_y = jax.random.randint(keys[2], (NETS,), 0, GY)
    width_y = jax.random.randint(keys[3], (NETS,), 1, SPAN_Y + 1)
    end_x = jnp.minimum(start_x + width_x - 1, GX - 1)
    end_y = jnp.minimum(start_y + width_y - 1, GY - 1)
    return jnp.stack([start_x, end_x, start_y, end_y]).astype(jnp.int32)


def set_ends(values, stream_key, low, largest):
    index_at = [jax.random.randint(jax.random.fold_in(stream_key, axis), (), 0, length) for axis, length in enumerate(values.shape)]
    main_axis = values.shape.index(max(values.shape))
    next_to = index_at[:main_axis] + [(index_at[main_axis] + 1) % values.shape[main_axis]] + index_at[main_axis + 1:]
    return values.at[tuple(index_at)].set(low).at[tuple(next_to)].set(largest)


def steps_of(own_key, dims, shards, smallest, high):
    def one(axis_at, shards_of):
        draws = jax.random.uniform(jax.random.fold_in(jax.random.fold_in(own_key, 6), axis_at), (shards_of,), jnp.float32, smallest / len(shards), high / len(shards))
        return jnp.repeat(jnp.exp(draws), dims[axis_at] // shards_of).reshape((-1,) + (1,) * (len(dims) - axis_at - 1))

    loudness = one(*shards[0])
    for cut in shards[1:]:
        loudness = loudness * one(*cut)
    return loudness


def setup_inputs(seed: int = 0) -> dict:
    key_list = jax.random.split(jax.random.key(seed), 6)
    return {
        "boxes": draw_boxes(jax.random.fold_in(key_list[5], 71), 0),
        "pins": set_ends(jax.random.randint(key_list[1], (NETS,), 2, 65), jax.random.fold_in(key_list[1], 1), 2, 64).astype(jnp.int32),
        "capacity": jnp.clip(jnp.exp(math.log(12.0) - 1.0986123 * jax.random.uniform(key_list[2], (GY, GX), jnp.float32) ** steps_of(key_list[2], (GY, GX), ((0, 4), (1, 8)), -0.2, 0.2)), 4.0, 12.0),
        "cell_bin": set_ends(jax.random.randint(key_list[3], (N_ROW, N_COL * CELLS_DEV), 0, TILE_R * TILE_C), jax.random.fold_in(key_list[3], 1), 0, (TILE_R * TILE_C) - 1).astype(jnp.int32),
        "cell_area": jnp.clip(jnp.exp(math.log(10.0) - 2.3025851 * jax.random.uniform(key_list[4], (N_ROW, N_COL * CELLS_DEV), jnp.float32) ** steps_of(key_list[4], (N_ROW, N_COL * CELLS_DEV), ((0, 4), (1, 8)), -0.2, 0.2)), 1.0, 10.0),
    }


def net_weights(boxes, pins):
    span_x = (boxes[1] - boxes[0] + 1).astype(jnp.float32)
    span_y = (boxes[3] - boxes[2] + 1).astype(jnp.float32)
    weight = jnp.log(pins.astype(jnp.float32)) * (span_x + span_y) / (span_x * span_y)
    return weight.astype(jnp.bfloat16).astype(jnp.float32)


def reference(boxes, pins, capacity, cell_bin, cell_area):
    weight = net_weights(boxes, pins)
    first_x, last_x, first_y, last_y = boxes[0], boxes[1], boxes[2], boxes[3]
    corner = jnp.zeros((GY + 1, GX + 1), jnp.float32)
    corner = corner.at[first_y, first_x].add(weight)
    corner = corner.at[first_y, last_x + 1].add(-weight)
    corner = corner.at[last_y + 1, first_x].add(-weight)
    corner = corner.at[last_y + 1, last_x + 1].add(weight)
    rudy = jnp.cumsum(jnp.cumsum(corner, axis=0), axis=1)[:GY, :GX]
    excess = jnp.maximum(rudy - capacity, 0.0)
    prefix = jnp.cumsum(excess, axis=0)
    inflation = 1.0 + 2.0 * prefix / GY
    tile_row = jnp.arange(N_ROW, dtype=jnp.int32)[:, None]
    position = jnp.arange(N_COL * CELLS_DEV, dtype=jnp.int32)[None, :]
    bin_row = tile_row * TILE_R + cell_bin // TILE_C
    bin_col = (position // CELLS_DEV) * TILE_C + cell_bin % TILE_C
    grown = cell_area * inflation[bin_row, bin_col]
    cell_sizes = grown * (jnp.sum(cell_area) / jnp.sum(grown))
    return rudy, inflation, cell_sizes
```

```python
import functools

import jax
import jax.numpy as jnp
from jax import lax
from jax.experimental import pallas as pl
from jax.experimental.pallas import tpu as pltpu
from jax.sharding import PartitionSpec as P

MESH = pl.DeviceIdType.MESH
F32 = jnp.float32
I16 = jnp.int16
F8 = jnp.float8_e4m3fn
BF16 = jnp.bfloat16
NT = (((1,), (1,)), ((), ()))
NN = (((1,), (0,)), ((), ()))


def split2(value):
    high = value.astype(BF16)
    return high, (value - high.astype(F32)).astype(BF16)


def kernel(
    n_row, n_col,
    boxes_hbm, pins_hbm, cap_hbm, bin_hbm, area_hbm,
    acc, within_ref, size_ref, final_ref,
    boxes_ref, pins_ref, cap_ref, bin_ref, area_ref,
    held_box, held_weight, own_weight, suffix, below_out, below_in, msg, col_out, col_in, looked,
    box_send, box_recv, weight_send, weight_recv, fbox_send, fweight_send,
    below_send, below_recv, col_send, col_recv, msg_send, msg_recv, load_sem, sums,
):
    rows, cols = acc.shape
    nets = boxes_ref.shape[1]
    cells = bin_ref.shape[1]
    n_chip = n_col // 2
    row = lax.axis_index("row")
    col = lax.axis_index("col")
    chip, core = col // 2, col % 2
    partner = chip * 2 + (1 - core)
    me = row * n_col + col

    def chip_at(offset):
        return lax.rem(chip + offset, n_chip)

    both_sides = jnp.minimum(chip, n_chip - 1 - chip)
    longer = jnp.where(chip < n_chip - 1 - chip, 1, -1)

    def nearest(step):
        turn = jnp.where(lax.rem(step, 2) == 1, 1, -1) * ((step + 1) // 2)
        return chip + jnp.where(step <= 2 * both_sides, turn, longer * (step - both_sides))

    barrier = pltpu.get_barrier_semaphore()
    for offset in range(1, n_chip):
        pl.semaphore_signal(
            barrier, inc=1, device_id=(row, chip_at(offset) * 2 + core), device_id_type=MESH
        )
    pl.semaphore_signal(barrier, inc=1, device_id=(row, partner), device_id_type=MESH)
    for offset in range(1, n_row):
        pl.semaphore_signal(
            barrier, inc=1, device_id=(lax.rem(row + offset, n_row), col), device_id_type=MESH
        )

    loads = [
        pltpu.make_async_copy(source, target, load_sem.at[index])
        for index, (source, target) in enumerate(
            [(boxes_hbm, boxes_ref), (pins_hbm, pins_ref), (bin_hbm, bin_ref), (area_hbm, area_ref), (cap_hbm, cap_ref)]
        )
    ]
    for copy in loads:
        copy.start()
    loads[0].wait()
    loads[1].wait()

    span_x = (boxes_ref[1:2, :] - boxes_ref[0:1, :] + 1).astype(F32)
    span_y = (boxes_ref[3:4, :] - boxes_ref[2:3, :] + 1).astype(F32)
    weight = jnp.log(pins_ref[...].astype(F32)) * (span_x + span_y) / (span_x * span_y)
    weight = weight.astype(BF16).astype(F32)
    own_weight[...] = weight
    held_weight[col] = weight
    held_box[col] = boxes_ref[...]

    pl.semaphore_wait(barrier, n_chip + n_row - 1)

    def pair(source, weight_source, slot, target, sems, index):
        first = pltpu.make_async_remote_copy(
            src_ref=source, dst_ref=held_box.at[slot], send_sem=sems[0].at[index],
            recv_sem=box_recv.at[slot], device_id=(row, target), device_id_type=MESH,
        )
        second = pltpu.make_async_remote_copy(
            src_ref=weight_source, dst_ref=held_weight.at[slot], send_sem=sems[1].at[index],
            recv_sem=weight_recv.at[slot], device_id=(row, target), device_id_type=MESH,
        )
        return first, second

    def own_copies():
        order = []
        for step in range(1, n_chip):
            order.append(nearest(step) * 2 + core)
        order.append(partner)
        made = []
        for target in order:
            made += pair(boxes_ref, own_weight, col, target, (box_send, weight_send), target)
        return made

    for copy in own_copies():
        copy.start()

    loads[2].wait()
    loads[3].wait()

    def cell_block(index, size):
        at = pl.ds(index * size, size)
        value = bin_ref[:, at]
        return lax.shift_right_logical(value, cols.bit_length() - 1), value & (cols - 1), area_ref[:, at]

    block = 512
    one, zero = jnp.ones((), BF16), jnp.zeros((), BF16)

    def iota(length, width=block):
        return lax.broadcasted_iota(jnp.int32, (length, width), 0).astype(I16)

    total = jnp.zeros((rows, 2 * cols), F32)
    for index in range(cells // block):
        bin_row, bin_col, area = cell_block(index, block)
        at_or_below = jnp.where(iota(rows) <= bin_row.astype(I16), one, zero)
        high, low = split2(area)
        same = iota(cols) == bin_col.astype(I16)
        table = jnp.concatenate([jnp.where(same, high, zero), jnp.where(same, low, zero)], axis=0)
        total += lax.dot_general(at_or_below, table, NT, preferred_element_type=F32)
    suffix[...] = total[:, :cols] + total[:, cols:]
    below_out[...] = jnp.broadcast_to(suffix[0:1, :], below_out.shape)

    def below_copies():
        made = []
        for offset in range(1, n_row):
            target = lax.rem(row + offset, n_row)
            made.append(
                pltpu.make_async_remote_copy(
                    src_ref=below_out, dst_ref=below_in.at[row], send_sem=below_send.at[target],
                    recv_sem=below_recv.at[row], device_id=(target, col), device_id_type=MESH,
                )
            )
        return made

    for copy in below_copies():
        copy.start()

    row_start = row * rows
    col_start = col * cols
    sums[...] = jnp.zeros_like(sums)

    def raster(slot):
        x0, x1 = held_box[slot, 0:1, :], held_box[slot, 1:2, :]
        y0, y1 = held_box[slot, 2:3, :], held_box[slot, 3:4, :]
        scaled = held_weight[slot, :, :] * 16.0
        high = scaled.astype(F8)
        low = ((scaled - high.astype(F32)) * 16.0).astype(F8)
        low_end = jnp.int16(-32768)
        ys, xs = iota(rows, nets) + low_end, iota(cols, nets) + low_end
        down = ys - (y0 - row_start).astype(I16) <= (y1 - y0 - 32768).astype(I16)
        across = xs - (x0 - col_start).astype(I16) <= (x1 - x0 - 32768).astype(I16)
        one8, zero8 = jnp.ones((rows, nets), F8), jnp.zeros((rows, nets), F8)
        weighted = jnp.concatenate(
            [jnp.where(across, jnp.broadcast_to(part, (cols, nets)), zero8[:cols]) for part in (high, low)], axis=0
        )
        sums[...] += lax.dot_general(
            jnp.where(down, one8, zero8), weighted, NT, preferred_element_type=F32
        )

    raster(col)

    def wait_pair(slot):
        first, second = pair(held_box.at[slot], held_weight.at[slot], slot, partner, (fbox_send, fweight_send), slot)
        first.wait_recv()
        second.wait_recv()

    wait_pair(partner)
    raster(partner)

    def forward(source):
        mine = source * 2 + core
        return pair(
            held_box.at[mine], held_weight.at[mine], mine, partner, (fbox_send, fweight_send), mine
        )

    def pass_on(step):
        source = nearest(step)
        wait_pair(source * 2 + core)
        for copy in forward(source):
            copy.start()

    def finish_source(step):
        other = nearest(step) * 2 + (1 - core)
        wait_pair(other)
        raster(other)

    def step(index, carry):
        pass_on(index)
        finish_source(index - 1)
        raster(nearest(index) * 2 + core)
        return carry

    if n_chip > 1:
        pass_on(1)
        raster(nearest(1) * 2 + core)
        lax.fori_loop(2, n_chip, step, 0)
        finish_source(n_chip - 1)
    for index in range(1, n_chip):
        for copy in forward(nearest(index)):
            copy.wait_send()

    for copy in below_copies():
        copy.wait_send()
    for offset in range(1, n_row):
        source = lax.rem(row + offset, n_row)
        pltpu.make_async_remote_copy(
            src_ref=below_out, dst_ref=below_in.at[source], send_sem=below_send.at[source],
            recv_sem=below_recv.at[source], device_id=(source, col), device_id_type=MESH,
        ).wait_recv()
    below = jnp.zeros((1, cols), F32)
    for source in range(n_row):
        below += jnp.where(source > row, below_in[source, 0:1, :], jnp.zeros((), F32))

    loads[4].wait()
    acc[...] = sums[:, :cols] * (1.0 / 16.0) + sums[:, cols:] * (1.0 / 256.0)
    excess = jnp.maximum(acc[...] - cap_ref[...], 0.0)
    col_out[...] = jnp.sum(excess, axis=0, keepdims=True)
    growth = jnp.sum(excess * (suffix[...] + below), axis=0, keepdims=True)
    area_lanes = suffix[0:1, :]
    half = cols // 2
    lanes = lax.broadcasted_iota(jnp.int32, (1, cols), 1)
    growth = growth + pltpu.roll(growth, half, 1)
    area_lanes = area_lanes + pltpu.roll(area_lanes, half, 1)
    msg[me] = jnp.where(lanes < half, growth, area_lanes)

    def message(row_step, col_step):
        target = (lax.rem(row + row_step, n_row), lax.rem(col + col_step, n_col))
        return pltpu.make_async_remote_copy(
            src_ref=msg.at[me], dst_ref=msg.at[me], send_sem=msg_send, recv_sem=msg_recv,
            device_id=target, device_id_type=MESH,
        )

    def far(step):
        row_step, col_step = step
        return -(min(row_step, n_row - row_step) + min(col_step, n_col - col_step))

    steps = [(a, b) for a in range(n_row) for b in range(n_col) if a or b]
    for step in sorted(steps, key=far):
        message(*step).start()

    def column_copy(offset):
        target = lax.rem(row + offset, n_row)
        return pltpu.make_async_remote_copy(
            src_ref=col_out, dst_ref=col_in.at[row], send_sem=col_send.at[target],
            recv_sem=col_recv.at[row], device_id=(target, col), device_id_type=MESH,
        )

    for offset in range(1, n_row):
        column_copy(offset).start()

    high, low = split2(excess)
    lower = jnp.where(
        lax.broadcasted_iota(jnp.int32, (rows, rows), 0).astype(I16)
        >= lax.broadcasted_iota(jnp.int32, (rows, rows), 1).astype(I16),
        one, zero,
    )
    both = lax.dot_general(
        lower, jnp.concatenate([high, low], axis=1), NN, preferred_element_type=F32
    )
    within = both[:, :cols] + both[:, cols:]
    within_ref[...] = within
    turned = within.T
    high, low = split2(turned)
    table = jnp.concatenate([high, low], axis=0)
    columns = lax.broadcasted_iota(jnp.int32, (cols, block), 0)
    for index in range(cells // block):
        bin_row, bin_col, _ = cell_block(index, block)
        same = jnp.where(iota(rows) == bin_row.astype(I16), one, zero)
        got = lax.dot_general(table, same, NN, preferred_element_type=F32)
        got = jnp.where(columns == bin_col, got[:cols] + got[cols:], 0.0)
        looked[:, pl.ds(index * block, block)] = jnp.sum(got, axis=0, keepdims=True)

    for copy in own_copies():
        copy.wait_send()
    carried = jnp.zeros((1, cols), F32)
    for offset in range(1, n_row):
        column_copy(offset).wait_send()
        source = lax.rem(row + offset, n_row)
        pltpu.make_async_remote_copy(
            src_ref=col_out, dst_ref=col_in.at[source], send_sem=col_send.at[source],
            recv_sem=col_recv.at[source], device_id=(source, col), device_id_type=MESH,
        ).wait_recv()
    for source in range(n_row):
        carried += jnp.where(source < row, col_in[source], jnp.zeros((), F32))
    scale = 2.0 / (rows * n_row)
    turned_carry = jnp.broadcast_to(carried, (8, cols)).T[:, 0:1]
    for index in range(cells // block):
        at = pl.ds(index * block, block)
        _, bin_col, area = cell_block(index, block)
        got = jnp.where(columns == bin_col, turned_carry, 0.0)
        got = looked[:, at] + jnp.sum(got, axis=0, keepdims=True)
        looked[:, at] = area * (1.0 + scale * got)
    final_ref[...] = jnp.broadcast_to(1.0 + scale * carried, final_ref.shape)

    total_dev = n_row * n_col
    everything = pltpu.make_async_remote_copy(
        src_ref=msg.at[pl.ds(0, total_dev - 1)], dst_ref=msg.at[pl.ds(0, total_dev - 1)],
        send_sem=msg_send, recv_sem=msg_recv, device_id=(row, partner), device_id_type=MESH,
    )
    everything.wait()
    sums = jnp.sum(msg[...], axis=0)
    area_total = jnp.sum(jnp.where(lanes < half, 0.0, sums), axis=1, keepdims=True)
    growth_total = jnp.sum(jnp.where(lanes < half, sums, 0.0), axis=1, keepdims=True)
    size_ref[...] = looked[...] * (area_total / (area_total + scale * growth_total))


def finish(scale, rudy, within, size, final, rudy_hbm, infl_hbm, size_hbm, infl, sems):
    first = pltpu.make_async_copy(rudy, rudy_hbm, sems.at[0])
    second = pltpu.make_async_copy(size, size_hbm, sems.at[1])
    third = pltpu.make_async_copy(infl, infl_hbm, sems.at[2])
    first.start()
    second.start()
    infl[...] = final[0:1, :] + scale * within[...]
    third.start()
    first.wait()
    second.wait()
    third.wait()


def solution(mesh):
    n_row, n_col = mesh.shape["row"], mesh.shape["col"]

    def per_device(boxes, pins, capacity, cell_bin, cell_area):
        rows, cols = capacity.shape
        nets = boxes.shape[1]
        cells = cell_bin.shape[1]
        vmem = pl.BlockSpec(memory_space=pltpu.VMEM)
        hbm = pl.BlockSpec(memory_space=pl.ANY)
        dma = pltpu.SemaphoreType.DMA
        rudy, within, size, final = pl.pallas_call(
            functools.partial(kernel, n_row, n_col),
            out_shape=(
                pltpu.VMEM((rows, cols), F32),
                pltpu.VMEM((rows, cols), F32),
                pltpu.VMEM((1, cells), F32),
                pltpu.VMEM((8, cols), F32),
            ),
            in_specs=[hbm] * 5,
            out_specs=(vmem,) * 4,
            scratch_shapes=[
                pltpu.VMEM((4, nets), jnp.int32),
                pltpu.VMEM((1, nets), jnp.int32),
                pltpu.VMEM((rows, cols), F32),
                pltpu.VMEM((1, cells), jnp.int32),
                pltpu.VMEM((1, cells), F32),
                pltpu.VMEM((n_col, 4, nets), jnp.int32),
                pltpu.VMEM((n_col, 1, nets), F32),
                pltpu.VMEM((1, nets), F32),
                pltpu.VMEM((rows, cols), F32),
                pltpu.VMEM((1, cols), F32),
                pltpu.VMEM((n_row, 1, cols), F32),
                pltpu.VMEM((n_row * n_col, 1, cols), F32),
                pltpu.VMEM((1, cols), F32),
                pltpu.VMEM((n_row, 1, cols), F32),
                pltpu.VMEM((1, cells), F32),
                dma((n_col,)), dma((n_col,)), dma((n_col,)), dma((n_col,)),
                dma((n_col,)), dma((n_col,)),
                dma((n_row,)), dma((n_row,)), dma((n_row,)), dma((n_row,)), dma, dma, dma((5,)),
                pltpu.VMEM((rows, 2 * cols), F32),
            ],
            compiler_params=pltpu.CompilerParams(
                collective_id=0, has_side_effects=True,
            ),
        )(boxes, pins[None, :], capacity, cell_bin, cell_area)
        return pl.pallas_call(
            functools.partial(finish, 2.0 / (rows * n_row)),
            out_shape=(
                jax.ShapeDtypeStruct((rows, cols), F32),
                jax.ShapeDtypeStruct((rows, cols), F32),
                jax.ShapeDtypeStruct((1, cells), F32),
            ),
            in_specs=[vmem] * 4,
            out_specs=(hbm,) * 3,
            scratch_shapes=[pltpu.VMEM((rows, cols), F32), dma((3,))],
        )(*[pltpu.with_memory_space_constraint(value, pltpu.VMEM) for value in (rudy, within, size, final)])

    in_specs = (P(None, "col"), P("col"), P("row", "col"), P("row", "col"), P("row", "col"))
    out_specs = (P("row", "col"), P("row", "col"), P("row", "col"))
    return jax.shard_map(
        per_device, mesh=mesh, in_specs=in_specs, out_specs=out_specs, check_vma=False
    )
```

```python
import functools

import jax
import jax.numpy as jnp
from jax import lax
from jax.experimental import pallas as pl
from jax.experimental.pallas import tpu as pltpu
from jax.sharding import PartitionSpec as P

MESH = pl.DeviceIdType.MESH
F32 = jnp.float32
I16 = jnp.int16
F8 = jnp.float8_e4m3fn
BF16 = jnp.bfloat16
NT = (((1,), (1,)), ((), ()))
NN = (((1,), (0,)), ((), ()))


def split2(value):
    high = value.astype(BF16)
    return high, (value - high.astype(F32)).astype(BF16)


def kernel(
    n_row, n_col,
    boxes_hbm, pins_hbm, cap_hbm, bin_hbm, area_hbm,
    acc, within_ref, size_ref, final_ref,
    boxes_ref, pins_ref, cap_ref, bin_ref, area_ref,
    held_box, held_weight, own_weight, suffix, below_out, below_in, msg, col_out, col_in, looked,
    box_send, box_recv, weight_send, weight_recv, fbox_send, fweight_send, token, far,
    below_send, below_recv, col_send, col_recv, msg_send, msg_recv, load_sem, table, *units,
):
    sums, looks = units[:2], units[2:]
    rows, cols = acc.shape
    nets = boxes_ref.shape[1]
    cells = bin_ref.shape[1]
    n_chip = n_col // 2
    row = lax.axis_index("row")
    col = lax.axis_index("col")
    chip, core = col // 2, col % 2
    partner = chip * 2 + (1 - core)
    me = row * n_col + col

    def chip_at(offset):
        return lax.rem(chip + offset, n_chip)

    both_sides = jnp.minimum(chip, n_chip - 1 - chip)
    longer = jnp.where(chip < n_chip - 1 - chip, 1, -1)

    def nearest(step):
        turn = jnp.where(lax.rem(step, 2) == 1, 1, -1) * ((step + 1) // 2)
        return chip + jnp.where(step <= 2 * both_sides, turn, longer * (step - both_sides))

    reach = min(2, n_chip - 1)
    flips = [1 << bit for bit in range(n_row.bit_length() - 1)]

    def flipped(mask):
        other = row
        for flip in flips:
            if mask & flip:
                other = other + flip * (1 - 2 * (row // flip % 2))
        return other

    def along(offsets, act):
        for offset in offsets:
            target = chip + offset

            @pl.when((target >= 0) & (target < n_chip))
            def _():
                act(offset + n_chip, target * 2 + core)

    before = range(1 - n_chip, 0)
    after = range(reach, 0, -1)
    beyond = range(n_chip - 1, reach, -1)
    waits_far = chip < n_chip - 1 - reach
    tells_far = (chip > 0) & (chip < n_chip - reach)

    barrier = pltpu.get_barrier_semaphore()

    def greet(target_row, target_col):
        pl.semaphore_signal(barrier, inc=1, device_id=(target_row, target_col), device_id_type=MESH)

    along([-offset for offset in (*after, *before)], lambda index, target: greet(row, target))
    greet(row, partner)
    for flip in flips:
        greet(flipped(flip), col)

    def tell_far():
        target = jnp.maximum(chip - 1, 0) * 2 + core
        pl.semaphore_signal(far, inc=1, device_id=(row, target), device_id_type=MESH)

    loads = [
        pltpu.make_async_copy(source, target, load_sem.at[index])
        for index, (source, target) in enumerate(
            [(boxes_hbm, boxes_ref), (pins_hbm, pins_ref), (bin_hbm, bin_ref), (area_hbm, area_ref), (cap_hbm, cap_ref)]
        )
    ]
    for copy in loads:
        copy.start()
    for unit in (*sums, *looks):
        pltpu.matmul_pop(unit)
    loads[0].wait()
    loads[1].wait()

    span_x = (boxes_ref[1:2, :] - boxes_ref[0:1, :] + 1).astype(F32)
    span_y = (boxes_ref[3:4, :] - boxes_ref[2:3, :] + 1).astype(F32)
    weight = jnp.log(pins_ref[...].astype(F32)) * (span_x + span_y) / (span_x * span_y)
    weight = weight.astype(BF16).astype(F32)
    own_weight[...] = weight
    held_weight[col] = weight
    held_box[col] = boxes_ref[...]

    around = chip + jnp.minimum(n_chip - 1 - chip, reach)
    pl.semaphore_wait(barrier, around + 1 + len(flips))
    pl.when(tells_far & jnp.logical_not(waits_far))(tell_far)

    def pair(source, weight_source, slot, target, sems, index):
        first = pltpu.make_async_remote_copy(
            src_ref=source, dst_ref=held_box.at[slot], send_sem=sems[0].at[index],
            recv_sem=box_recv.at[slot], device_id=(row, target), device_id_type=MESH,
        )
        second = pltpu.make_async_remote_copy(
            src_ref=weight_source, dst_ref=held_weight.at[slot], send_sem=sems[1].at[index],
            recv_sem=weight_recv.at[slot], device_id=(row, target), device_id_type=MESH,
        )
        return first, second

    def own_copies(offsets, act):
        def one(index, target):
            for copy in pair(boxes_ref, own_weight, col, target, (box_send, weight_send), index):
                act(copy)

        if offsets:
            along(offsets, one)
        else:
            one(n_chip, partner)

    def start(copy):
        copy.start()

    def sent(copy):
        copy.wait_send()

    own_copies(before, start)
    own_copies(after, start)
    own_copies((), start)

    loads[2].wait()
    loads[3].wait()

    def cell_block(index, size):
        at = pl.ds(index * size, size)
        value = bin_ref[:, at]
        return lax.shift_right_logical(value, cols.bit_length() - 1), value & (cols - 1), area_ref[:, at]

    block = 256
    one, zero = jnp.ones((), BF16), jnp.zeros((), BF16)

    def iota(length, width=block):
        return lax.broadcasted_iota(jnp.int32, (length, width), 0).astype(I16)

    for index in range(cells // block):
        bin_row, bin_col, area = cell_block(index, block)
        unit, stage = index % 2, index // 2 % 2
        at_or_below = jnp.where(iota(rows) <= bin_row.astype(I16), one, zero)
        high, low = split2(area)
        same = iota(cols) == bin_col.astype(I16)
        held = jnp.concatenate([jnp.where(same, high, zero), jnp.where(same, low, zero)], axis=0)
        pltpu.matmul_push_rhs(held, staging_register=stage, mxu_index=unit, transpose=True)
        pltpu.matmul_acc_lhs(sums[unit], at_or_below, load_staged_rhs=stage)
    total = pltpu.matmul_pop(sums[0]) + pltpu.matmul_pop(sums[1])
    suffix[...] = total[:, :cols] + total[:, cols:]
    below_out[0] = suffix[0:1, :]

    def below_copy(bit):
        return pltpu.make_async_remote_copy(
            src_ref=below_out.at[bit], dst_ref=below_in.at[bit], send_sem=below_send.at[bit],
            recv_sem=below_recv.at[bit], device_id=(flipped(flips[bit]), col), device_id_type=MESH,
        )

    below_copy(0).start()

    @pl.when(waits_far)
    def _():
        pl.semaphore_wait(far, 1)
        own_copies(beyond, start)
        pl.when(tells_far)(tell_far)

    def take_below(bit):
        below_copy(bit).wait_recv()
        if bit + 1 < len(flips):
            below_out[bit + 1] = below_out[bit] + below_in[bit]
            below_copy(bit + 1).start()

    row_start = row * rows
    col_start = col * cols
    one8, zero8 = jnp.ones((rows, block), F8), jnp.zeros((rows, block), F8)
    low_end = jnp.int16(-32768)

    def raster(slot):
        ys, xs = iota(rows) + low_end, iota(cols) + low_end
        for index in range(nets // block):
            at = pl.ds(index * block, block)
            unit, stage = index % 2, index // 2 % 2
            x0, x1 = held_box[slot, 0:1, at], held_box[slot, 1:2, at]
            y0, y1 = held_box[slot, 2:3, at], held_box[slot, 3:4, at]
            scaled = held_weight[slot, :, at] * 16.0
            high = scaled.astype(F8)
            low = ((scaled - high.astype(F32)) * 16.0).astype(F8)
            down = ys - (y0 - row_start).astype(I16) <= (y1 - y0 - 32768).astype(I16)
            across = xs - (x0 - col_start).astype(I16) <= (x1 - x0 - 32768).astype(I16)
            weighted = jnp.concatenate(
                [jnp.where(across, jnp.broadcast_to(part, (cols, block)), zero8[:cols]) for part in (high, low)], axis=0
            )
            pltpu.matmul_push_rhs(weighted, staging_register=stage, mxu_index=unit, transpose=True)
            pltpu.matmul_acc_lhs(sums[unit], jnp.where(down, one8, zero8), load_staged_rhs=stage)

    raster(col)

    def wait_pair(slot):
        first, second = pair(held_box.at[slot], held_weight.at[slot], slot, partner, (fbox_send, fweight_send), slot)
        first.wait_recv()
        second.wait_recv()

    wait_pair(partner)
    raster(partner)

    def forward(source):
        mine = source * 2 + core
        return pair(
            held_box.at[mine], held_weight.at[mine], mine, partner, (fbox_send, fweight_send), mine
        )

    def pass_on(step):
        source = nearest(step)
        wait_pair(source * 2 + core)
        for copy in forward(source):
            copy.start()

    def finish_source(step, then=lambda: None):
        other = nearest(step) * 2 + (1 - core)
        wait_pair(other)
        then()
        raster(other)

    far_rows = [mask for mask in range(1, n_row) if mask not in flips]

    def tell_far_rows():
        for bit in range(len(flips) - 1):
            take_below(bit)
        for mask in far_rows:
            pl.semaphore_signal(token, inc=1, device_id=(flipped(mask), col), device_id_type=MESH)

    def step(index, carry):
        pass_on(index)
        finish_source(index - 1)
        raster(nearest(index) * 2 + core)
        return carry

    pass_on(1)
    raster(nearest(1) * 2 + core)
    pass_on(2)
    finish_source(1, tell_far_rows)
    raster(nearest(2) * 2 + core)
    lax.fori_loop(3, n_chip, step, 0)
    finish_source(n_chip - 1)
    for index in range(1, n_chip):
        for copy in forward(nearest(index)):
            copy.wait_send()
    take_below(len(flips) - 1)
    for bit in range(len(flips)):
        below_copy(bit).wait_send()
    below = jnp.zeros((1, cols), F32)
    for bit, flip in enumerate(flips):
        below += jnp.where(row // flip % 2 == 0, below_in[bit], jnp.zeros((), F32))
    pl.semaphore_wait(token, len(far_rows))

    loads[4].wait()
    both = pltpu.matmul_pop(sums[0]) + pltpu.matmul_pop(sums[1])
    acc[...] = both[:, :cols] * (1.0 / 16.0) + both[:, cols:] * (1.0 / 256.0)
    excess = jnp.maximum(acc[...] - cap_ref[...], 0.0)
    col_out[...] = jnp.sum(excess, axis=0, keepdims=True)
    growth = jnp.sum(excess * (suffix[...] + below), axis=0, keepdims=True)
    area_lanes = suffix[0:1, :]
    half = cols // 2
    lanes = lax.broadcasted_iota(jnp.int32, (1, cols), 1)
    growth = growth + pltpu.roll(growth, half, 1)
    area_lanes = area_lanes + pltpu.roll(area_lanes, half, 1)
    msg[me] = jnp.where(lanes < half, growth, area_lanes)

    def message(row_step, col_step):
        target = (lax.rem(row + row_step, n_row), lax.rem(col + col_step, n_col))
        return pltpu.make_async_remote_copy(
            src_ref=msg.at[me], dst_ref=msg.at[me], send_sem=msg_send, recv_sem=msg_recv,
            device_id=target, device_id_type=MESH,
        )

    def far(step):
        row_step, col_step = step
        return -(min(row_step, n_row - row_step) + min(col_step, n_col - col_step))

    def column_copy(offset):
        target = lax.rem(row + offset, n_row)
        return pltpu.make_async_remote_copy(
            src_ref=col_out, dst_ref=col_in.at[row], send_sem=col_send.at[target],
            recv_sem=col_recv.at[row], device_id=(target, col), device_id_type=MESH,
        )

    for offset in range(1, n_row):
        column_copy(offset).start()

    steps = [(a, b) for a in range(n_row) for b in range(n_col) if a or b]
    for step in sorted(steps, key=far):
        message(*step).start()

    parts = jnp.concatenate(split2(excess), axis=1)
    for index in range(rows // block):
        unit, stage = index % 2, index // 2 % 2
        above = lax.broadcasted_iota(jnp.int32, (rows, block), 1).astype(I16) + jnp.int16(index * block)
        lower = jnp.where(iota(rows) >= above, one, zero)
        pltpu.matmul_push_rhs(parts[index * block:(index + 1) * block], staging_register=stage, mxu_index=unit)
        pltpu.matmul_acc_lhs(sums[unit], lower, load_staged_rhs=stage)
    both = pltpu.matmul_pop(sums[0]) + pltpu.matmul_pop(sums[1])
    within = both[:, :cols] + both[:, cols:]
    within_ref[...] = within
    table[...] = jnp.concatenate(split2(within.T), axis=0)
    columns = lax.broadcasted_iota(jnp.int32, (cols, block), 0)
    for index in range(cells // block):
        bin_row, bin_col, _ = cell_block(index, block)
        unit = index % 2
        got = looks[index % len(looks)]
        for part in range(rows // block):
            at = pl.ds(part * block, block)
            same = jnp.where(iota(block) == (bin_row - part * block).astype(I16), one, zero)
            pltpu.matmul_push_rhs(same, staging_register=part % 2, mxu_index=unit)
            pltpu.matmul_acc_lhs(got, table[:, at], load_staged_rhs=part % 2)
        got = pltpu.matmul_pop(got)
        got = jnp.where(columns == bin_col, got[:cols] + got[cols:], 0.0)
        looked[:, pl.ds(index * block, block)] = jnp.sum(got, axis=0, keepdims=True)

    own_copies((*before, *after, *beyond), sent)
    own_copies((), sent)
    carried = jnp.zeros((1, cols), F32)
    for offset in range(1, n_row):
        column_copy(offset).wait_send()
        source = lax.rem(row + offset, n_row)
        pltpu.make_async_remote_copy(
            src_ref=col_out, dst_ref=col_in.at[source], send_sem=col_send.at[source],
            recv_sem=col_recv.at[source], device_id=(source, col), device_id_type=MESH,
        ).wait_recv()
    for source in range(n_row):
        carried += jnp.where(source < row, col_in[source], jnp.zeros((), F32))
    scale = 2.0 / (rows * n_row)
    turned_carry = jnp.broadcast_to(carried, (8, cols)).T[:, 0:1]
    for index in range(cells // block):
        at = pl.ds(index * block, block)
        _, bin_col, area = cell_block(index, block)
        got = jnp.where(columns == bin_col, turned_carry, 0.0)
        got = looked[:, at] + jnp.sum(got, axis=0, keepdims=True)
        looked[:, at] = area * (1.0 + scale * got)
    final_ref[...] = jnp.broadcast_to(1.0 + scale * carried, final_ref.shape)

    total_dev = n_row * n_col
    everything = pltpu.make_async_remote_copy(
        src_ref=msg.at[pl.ds(0, total_dev - 1)], dst_ref=msg.at[pl.ds(0, total_dev - 1)],
        send_sem=msg_send, recv_sem=msg_recv, device_id=(row, partner), device_id_type=MESH,
    )
    everything.wait()
    sums = jnp.sum(msg[...], axis=0)
    area_total = jnp.sum(jnp.where(lanes < half, 0.0, sums), axis=1, keepdims=True)
    growth_total = jnp.sum(jnp.where(lanes < half, sums, 0.0), axis=1, keepdims=True)
    size_ref[...] = looked[...] * (area_total / (area_total + scale * growth_total))


def with_units(body, *refs):
    rows, cols = refs[5].shape
    wide = 2 * cols
    pl.run_scoped(
        functools.partial(body, *refs),
        *[pltpu.ACC(unit)((rows, wide), F32) for unit in (0, 1)],
        *[pltpu.ACC(unit)((wide, wide), F32) for unit in (0, 1, 0, 1)],
    )


def finish(scale, rudy, within, size, final, rudy_hbm, infl_hbm, size_hbm, infl, sems):
    first = pltpu.make_async_copy(rudy, rudy_hbm, sems.at[0])
    second = pltpu.make_async_copy(size, size_hbm, sems.at[1])
    third = pltpu.make_async_copy(infl, infl_hbm, sems.at[2])
    first.start()
    second.start()
    infl[...] = final[0:1, :] + scale * within[...]
    third.start()
    first.wait()
    second.wait()
    third.wait()


def solution(mesh):
    n_row, n_col = mesh.shape["row"], mesh.shape["col"]

    def per_device(boxes, pins, capacity, cell_bin, cell_area):
        rows, cols = capacity.shape
        nets = boxes.shape[1]
        cells = cell_bin.shape[1]
        vmem = pl.BlockSpec(memory_space=pltpu.VMEM)
        hbm = pl.BlockSpec(memory_space=pl.ANY)
        dma = pltpu.SemaphoreType.DMA
        rudy, within, size, final = pl.pallas_call(
            functools.partial(with_units, functools.partial(kernel, n_row, n_col)),
            out_shape=(
                pltpu.VMEM((rows, cols), F32),
                pltpu.VMEM((rows, cols), F32),
                pltpu.VMEM((1, cells), F32),
                pltpu.VMEM((8, cols), F32),
            ),
            in_specs=[hbm] * 5,
            out_specs=(vmem,) * 4,
            scratch_shapes=[
                pltpu.VMEM((4, nets), jnp.int32),
                pltpu.VMEM((1, nets), jnp.int32),
                pltpu.VMEM((rows, cols), F32),
                pltpu.VMEM((1, cells), jnp.int32),
                pltpu.VMEM((1, cells), F32),
                pltpu.VMEM((n_col, 4, nets), jnp.int32),
                pltpu.VMEM((n_col, 1, nets), F32),
                pltpu.VMEM((1, nets), F32),
                pltpu.VMEM((rows, cols), F32),
                pltpu.VMEM((n_row, 1, cols), F32),
                pltpu.VMEM((n_row, 1, cols), F32),
                pltpu.VMEM((n_row * n_col, 1, cols), F32),
                pltpu.VMEM((1, cols), F32),
                pltpu.VMEM((n_row, 1, cols), F32),
                pltpu.VMEM((1, cells), F32),
                dma((n_col,)), dma((n_col,)), dma((n_col,)), dma((n_col,)),
                dma((n_col,)), dma((n_col,)), pltpu.SemaphoreType.REGULAR, pltpu.SemaphoreType.REGULAR,
                dma((n_row,)), dma((n_row,)), dma((n_row,)), dma((n_row,)), dma, dma, dma((5,)),
                pltpu.VMEM((2 * cols, rows), BF16),
            ],
            compiler_params=pltpu.CompilerParams(
                collective_id=0, has_side_effects=True,
            ),
        )(boxes, pins[None, :], capacity, cell_bin, cell_area)
        return pl.pallas_call(
            functools.partial(finish, 2.0 / (rows * n_row)),
            out_shape=(
                jax.ShapeDtypeStruct((rows, cols), F32),
                jax.ShapeDtypeStruct((rows, cols), F32),
                jax.ShapeDtypeStruct((1, cells), F32),
            ),
            in_specs=[vmem] * 4,
            out_specs=(hbm,) * 3,
            scratch_shapes=[pltpu.VMEM((rows, cols), F32), dma((3,))],
        )(*[pltpu.with_memory_space_constraint(value, pltpu.VMEM) for value in (rudy, within, size, final)])

    in_specs = (P(None, "col"), P("col"), P("row", "col"), P("row", "col"), P("row", "col"))
    out_specs = (P("row", "col"), P("row", "col"), P("row", "col"))
    return jax.shard_map(
        per_device, mesh=mesh, in_specs=in_specs, out_specs=out_specs, check_vma=False
    )
```

```python
import functools

import jax
import jax.numpy as jnp
from jax import lax
from jax.experimental import pallas as pl
from jax.experimental.pallas import tpu as pltpu
from jax.sharding import PartitionSpec as P

MESH = pl.DeviceIdType.MESH
F32 = jnp.float32
I16 = jnp.int16
F8 = jnp.float8_e4m3fn
BF16 = jnp.bfloat16
NT = (((1,), (1,)), ((), ()))
NN = (((1,), (0,)), ((), ()))


ORDER = ((1, 2, 3), (3, 0, 2), (0, 3, 1), (2, 1, 0))


def split2(value):
    high = value.astype(BF16)
    return high, (value - high.astype(F32)).astype(BF16)


def kernel(
    n_row, n_col,
    boxes_hbm, pins_hbm, cap_hbm, bin_hbm, area_hbm,
    acc, within_ref, size_ref, final_ref,
    boxes_ref, pins_ref, cap_ref, bin_ref, area_ref,
    held_box, held_weight, own_weight, suffix, below_out, below_in, msg, col_out, col_in, looked,
    box_send, weight_send, net_recv, token, far_in,
    below_send, below_recv, col_send, col_recv, msg_send, msg_recv, load_sem, table, *units,
):
    sums, looks = units[:2], units[2:]
    rows, cols = acc.shape
    nets = boxes_ref.shape[1]
    cells = bin_ref.shape[1]
    n_chip = n_col // 2
    row = lax.axis_index("row")
    col = lax.axis_index("col")
    chip, core = col // 2, col % 2
    partner = chip * 2 + (1 - core)
    me = row * n_col + col

    both_sides = jnp.minimum(chip, n_chip - 1 - chip)
    longer = jnp.where(chip < n_chip - 1 - chip, 1, -1)

    def nearest(step):
        turn = jnp.where(lax.rem(step, 2) == 1, 1, -1) * ((step + 1) // 2)
        return chip + jnp.where(step <= 2 * both_sides, turn, longer * (step - both_sides))

    def origin(step):
        if n_chip != len(ORDER):
            return nearest(step)
        return sum(jnp.where(chip == at, ORDER[at][step - 1], 0) for at in range(n_chip))

    reach = min(2, n_chip - 1)
    flips = [1 << bit for bit in range(n_row.bit_length() - 1)]

    def flipped(mask):
        other = row
        for flip in flips:
            if mask & flip:
                other = other + flip * (1 - 2 * (row // flip % 2))
        return other

    def along(offsets, act):
        for offset in offsets:
            target = chip + offset

            @pl.when((target >= 0) & (target < n_chip))
            def _():
                act(target * 2 + core)

    before = range(1 - n_chip, 0)
    after = range(reach, 0, -1)
    beyond = range(n_chip - 1, reach, -1)
    waits_far = chip < n_chip - 1 - reach
    tells_far = (chip > 0) & (chip < n_chip - reach)

    barrier = pltpu.get_barrier_semaphore()

    def greet(target_row, target_col):
        pl.semaphore_signal(barrier, inc=1, device_id=(target_row, target_col), device_id_type=MESH)

    along([-offset for offset in (*after, *before)], lambda target: greet(row, target))
    greet(row, partner)
    for flip in flips:
        greet(flipped(flip), col)

    def tell_far():
        target = jnp.maximum(chip - 1, 0) * 2 + core
        pl.semaphore_signal(far_in, inc=1, device_id=(row, target), device_id_type=MESH)

    sources = [(boxes_hbm, boxes_ref, 0), (pins_hbm, pins_ref, 0), (bin_hbm, bin_ref, 1), (area_hbm, area_ref, 1)]
    for source, target, index in (*sources, (cap_hbm, cap_ref, 2)):
        pltpu.make_async_copy(source, target, load_sem.at[index]).start()

    def landed(index, like):
        pltpu.make_async_copy(like, like, load_sem.at[index]).wait()

    net_rows = acc.at[pl.ds(0, 5 * nets // cols)]
    for unit in (*sums, *looks):
        pltpu.matmul_pop(unit)
    landed(0, net_rows)

    span_x = (boxes_ref[1:2, :] - boxes_ref[0:1, :] + 1).astype(F32)
    span_y = (boxes_ref[3:4, :] - boxes_ref[2:3, :] + 1).astype(F32)
    weight = jnp.log(pins_ref[...].astype(F32)) * (span_x + span_y) / (span_x * span_y)
    weight = weight.astype(BF16).astype(F32)
    own_weight[...] = weight
    held_weight[col] = weight
    held_box[col] = boxes_ref[...]

    around = chip + jnp.minimum(n_chip - 1 - chip, reach)
    pl.semaphore_wait(barrier, around + 1 + len(flips))
    pl.when(tells_far & jnp.logical_not(waits_far))(tell_far)

    def pair(source, weight_source, slot, target):
        return [
            pltpu.make_async_remote_copy(
                src_ref=src, dst_ref=held.at[slot], send_sem=send, recv_sem=net_recv.at[slot],
                device_id=(row, target), device_id_type=MESH,
            )
            for src, held, send in ((source, held_box, box_send), (weight_source, held_weight, weight_send))
        ]

    def send_own(target):
        for copy in pair(boxes_ref, own_weight, col, target):
            copy.start()

    along(before, send_own)
    along(after, send_own)
    send_own(partner)

    landed(1, held_weight.at[pl.ds(0, 2)])

    def cell_block(index, size):
        at = pl.ds(index * size, size)
        value = bin_ref[:, at]
        return lax.shift_right_logical(value, cols.bit_length() - 1), value & (cols - 1), area_ref[:, at]

    block = 256
    one, zero = jnp.ones((), BF16), jnp.zeros((), BF16)

    def iota(length, width=block):
        return lax.broadcasted_iota(jnp.int32, (length, width), 0).astype(I16)

    for index in range(cells // block):
        bin_row, bin_col, area = cell_block(index, block)
        unit, stage = index % 2, index // 2 % 2
        at_or_below = jnp.where(iota(rows) <= bin_row.astype(I16), one, zero)
        high, low = split2(area)
        same = iota(cols) == bin_col.astype(I16)
        held = jnp.concatenate([jnp.where(same, high, zero), jnp.where(same, low, zero)], axis=0)
        pltpu.matmul_push_rhs(held, staging_register=stage, mxu_index=unit, transpose=True)
        pltpu.matmul_acc_lhs(sums[unit], at_or_below, load_staged_rhs=stage)
    total = pltpu.matmul_pop(sums[0]) + pltpu.matmul_pop(sums[1])
    suffix[...] = total[:, :cols] + total[:, cols:]
    below_out[0] = suffix[0:1, :]
    msg[me, 1:2, :] = suffix[0:1, :]

    def below_copy(bit):
        return pltpu.make_async_remote_copy(
            src_ref=below_out.at[bit], dst_ref=below_in.at[bit], send_sem=below_send,
            recv_sem=below_recv.at[bit], device_id=(flipped(flips[bit]), col), device_id_type=MESH,
        )

    below_copy(0).start()

    @pl.when(waits_far)
    def _():
        pl.semaphore_wait(far_in, 1)
        along(beyond, send_own)
        pl.when(tells_far)(tell_far)

    def take_below(bit):
        below_copy(bit).wait_recv()
        if bit + 1 < len(flips):
            below_out[bit + 1] = below_out[bit] + below_in[bit]
            below_copy(bit + 1).start()

    row_start = row * rows
    col_start = col * cols
    one8, zero8 = jnp.ones((rows, block), F8), jnp.zeros((rows, block), F8)
    low_end = jnp.int16(-32768)

    def raster(slot):
        ys, xs = iota(rows) + low_end, iota(cols) + low_end
        for index in range(nets // block):
            at = pl.ds(index * block, block)
            unit, stage = index % 2, index // 2 % 2
            x0, x1 = held_box[slot, 0:1, at], held_box[slot, 1:2, at]
            y0, y1 = held_box[slot, 2:3, at], held_box[slot, 3:4, at]
            scaled = held_weight[slot, :, at] * 16.0
            high = scaled.astype(F8)
            low = ((scaled - high.astype(F32)) * 16.0).astype(F8)
            down = ys - (y0 - row_start).astype(I16) <= (y1 - y0 - 32768).astype(I16)
            across = xs - (x0 - col_start).astype(I16) <= (x1 - x0 - 32768).astype(I16)
            weighted = jnp.concatenate(
                [jnp.where(across, jnp.broadcast_to(part, (cols, block)), zero8[:cols]) for part in (high, low)], axis=0
            )
            pltpu.matmul_push_rhs(weighted, staging_register=stage, mxu_index=unit, transpose=True)
            pltpu.matmul_acc_lhs(sums[unit], jnp.where(down, one8, zero8), load_staged_rhs=stage)

    raster(col)

    def wait_pair(slot):
        pltpu.make_async_remote_copy(
            src_ref=net_rows, dst_ref=net_rows, send_sem=box_send, recv_sem=net_recv.at[slot],
            device_id=(row, partner), device_id_type=MESH,
        ).wait_recv()

    wait_pair(partner)
    raster(partner)

    def pass_on(step):
        slot = origin(step) * 2 + core
        wait_pair(slot)
        for copy in pair(held_box.at[slot], held_weight.at[slot], slot, partner):
            copy.start()

    def finish_source(step, then=lambda: None):
        other = origin(step) * 2 + (1 - core)
        wait_pair(other)
        then()
        raster(other)

    far_rows = [mask for mask in range(1, n_row) if mask not in flips]

    def tell_far_rows():
        for bit in range(len(flips) - 1):
            take_below(bit)
        for mask in far_rows:
            pl.semaphore_signal(token, inc=1, device_id=(flipped(mask), col), device_id_type=MESH)

    def step(index, carry):
        pass_on(index)
        finish_source(index - 1)
        raster(origin(index) * 2 + core)
        return carry

    pass_on(1)
    raster(origin(1) * 2 + core)
    pass_on(2)
    finish_source(1, tell_far_rows)
    raster(origin(2) * 2 + core)
    if n_chip == len(ORDER):
        for index in range(3, n_chip):
            step(index, 0)
    else:
        lax.fori_loop(3, n_chip, step, 0)
    finish_source(n_chip - 1)
    take_below(len(flips) - 1)
    below = jnp.zeros((1, cols), F32)
    for bit, flip in enumerate(flips):
        below += jnp.where(row // flip % 2 == 0, below_in[bit], jnp.zeros((), F32))
    pl.semaphore_wait(token, len(far_rows))

    landed(2, cap_ref)
    both = pltpu.matmul_pop(sums[0]) + pltpu.matmul_pop(sums[1])
    acc[...] = both[:, :cols] * (1.0 / 16.0) + both[:, cols:] * (1.0 / 256.0)
    excess = jnp.maximum(acc[...] - cap_ref[...], 0.0)
    col_out[...] = jnp.sum(excess, axis=0, keepdims=True)
    growth = jnp.sum(excess * (suffix[...] + below), axis=0, keepdims=True)
    msg[me, 0:1, :] = growth

    def column_copy(offset):
        target = lax.rem(row + offset, n_row)
        return pltpu.make_async_remote_copy(
            src_ref=col_out, dst_ref=col_in.at[row], send_sem=col_send, recv_sem=col_recv,
            device_id=(target, col), device_id_type=MESH,
        )

    for offset in range(1, n_row):
        column_copy(offset).start()

    def message(mask, step, side):
        target = (nearest(step) if step else chip) * 2 + (core if side else 1 - core)
        return pltpu.make_async_remote_copy(
            src_ref=msg.at[me], dst_ref=msg.at[me], send_sem=msg_send, recv_sem=msg_recv,
            device_id=(flipped(mask), target), device_id_type=MESH,
        )

    def hops(at):
        mask, step, _ = at
        return -(mask.bit_count() + step)

    everyone = [(mask, step, side) for mask in range(n_row) for step in range(n_chip) for side in (0, 1)]
    for at in sorted(everyone, key=hops):
        if at != (0, 0, 1):
            message(*at).start()

    parts = jnp.concatenate(split2(excess), axis=1)
    for index in range(rows // block):
        unit, stage = index % 2, index // 2 % 2
        above = lax.broadcasted_iota(jnp.int32, (rows, block), 1).astype(I16) + jnp.int16(index * block)
        lower = jnp.where(iota(rows) >= above, one, zero)
        pltpu.matmul_push_rhs(parts[index * block:(index + 1) * block], staging_register=stage, mxu_index=unit)
        pltpu.matmul_acc_lhs(sums[unit], lower, load_staged_rhs=stage)
    both = pltpu.matmul_pop(sums[0]) + pltpu.matmul_pop(sums[1])
    within = both[:, :cols] + both[:, cols:]
    within_ref[...] = within
    table[...] = jnp.concatenate(split2(within.T), axis=0)
    columns = lax.broadcasted_iota(jnp.int32, (cols, block), 0)
    for index in range(cells // block):
        bin_row, bin_col, _ = cell_block(index, block)
        unit = index % 2
        got = looks[index % len(looks)]
        for part in range(rows // block):
            at = pl.ds(part * block, block)
            same = jnp.where(iota(block) == (bin_row - part * block).astype(I16), one, zero)
            pltpu.matmul_push_rhs(same, staging_register=part % 2, mxu_index=unit)
            pltpu.matmul_acc_lhs(got, table[:, at], load_staged_rhs=part % 2)
        got = pltpu.matmul_pop(got)
        got = jnp.where(columns == bin_col, got[:cols] + got[cols:], 0.0)
        looked[:, pl.ds(index * block, block)] = jnp.sum(got, axis=0, keepdims=True)

    def drain(like, send, recv=None):
        copy = pltpu.make_async_remote_copy(
            src_ref=like, dst_ref=like, send_sem=send, recv_sem=col_recv if recv is None else recv,
            device_id=(row, partner), device_id_type=MESH,
        )
        copy.wait_send()
        if recv is not None:
            copy.wait_recv()

    drain(held_box.at[pl.ds(0, n_col - 1)], box_send)
    drain(held_weight.at[pl.ds(0, n_col - 1)], weight_send)
    drain(below_out.at[pl.ds(0, len(flips))], below_send)
    drain(col_in.at[pl.ds(0, n_row - 1)], col_send, col_recv)
    carried = jnp.zeros((1, cols), F32)
    for index in range(n_row):
        carried += jnp.where(index < row, col_in[index], jnp.zeros((), F32))
    scale = 2.0 / (rows * n_row)
    turned_carry = jnp.broadcast_to(carried, (8, cols)).T[:, 0:1]
    for index in range(cells // block):
        at = pl.ds(index * block, block)
        _, bin_col, area = cell_block(index, block)
        got = jnp.where(columns == bin_col, turned_carry, 0.0)
        got = looked[:, at] + jnp.sum(got, axis=0, keepdims=True)
        looked[:, at] = area * (1.0 + scale * got)
    final_ref[...] = jnp.broadcast_to(1.0 + scale * carried, final_ref.shape)

    drain(msg.at[pl.ds(0, n_row * n_col - 1)], msg_send, msg_recv)
    sums_all = jnp.sum(jnp.sum(msg[...], axis=0), axis=1, keepdims=True)
    growth_total, area_total = sums_all[0:1], sums_all[1:2]
    size_ref[...] = looked[...] * (area_total / (area_total + scale * growth_total))


def with_units(body, *refs):
    rows, cols = refs[5].shape
    wide = 2 * cols
    pl.run_scoped(
        functools.partial(body, *refs),
        *[pltpu.ACC(unit)((rows, wide), F32) for unit in (0, 1)],
        *[pltpu.ACC(unit)((wide, wide), F32) for unit in (0, 1, 0, 1)],
    )


def finish(scale, rudy, within, size, final, rudy_hbm, infl_hbm, size_hbm, infl, sems):
    first = pltpu.make_async_copy(rudy, rudy_hbm, sems.at[0])
    second = pltpu.make_async_copy(size, size_hbm, sems.at[1])
    third = pltpu.make_async_copy(infl, infl_hbm, sems.at[2])
    first.start()
    second.start()
    infl[...] = final[0:1, :] + scale * within[...]
    third.start()
    first.wait()
    second.wait()
    third.wait()


def solution(mesh):
    n_row, n_col = mesh.shape["row"], mesh.shape["col"]

    def per_device(boxes, pins, capacity, cell_bin, cell_area):
        rows, cols = capacity.shape
        nets = boxes.shape[1]
        cells = cell_bin.shape[1]
        vmem = pl.BlockSpec(memory_space=pltpu.VMEM)
        hbm = pl.BlockSpec(memory_space=pl.ANY)
        dma = pltpu.SemaphoreType.DMA
        rudy, within, size, final = pl.pallas_call(
            functools.partial(with_units, functools.partial(kernel, n_row, n_col)),
            out_shape=(
                pltpu.VMEM((rows, cols), F32),
                pltpu.VMEM((rows, cols), F32),
                pltpu.VMEM((1, cells), F32),
                pltpu.VMEM((8, cols), F32),
            ),
            in_specs=[hbm] * 5,
            out_specs=(vmem,) * 4,
            scratch_shapes=[
                pltpu.VMEM((4, nets), jnp.int32),
                pltpu.VMEM((1, nets), jnp.int32),
                pltpu.VMEM((rows, cols), F32),
                pltpu.VMEM((1, cells), jnp.int32),
                pltpu.VMEM((1, cells), F32),
                pltpu.VMEM((n_col, 4, nets), jnp.int32),
                pltpu.VMEM((n_col, 1, nets), F32),
                pltpu.VMEM((1, nets), F32),
                pltpu.VMEM((rows, cols), F32),
                pltpu.VMEM((n_row, 1, cols), F32),
                pltpu.VMEM((n_row, 1, cols), F32),
                pltpu.VMEM((n_row * n_col, 2, cols), F32),
                pltpu.VMEM((1, cols), F32),
                pltpu.VMEM((n_row, 1, cols), F32),
                pltpu.VMEM((1, cells), F32),
                dma, dma, dma((n_col,)), pltpu.SemaphoreType.REGULAR, pltpu.SemaphoreType.REGULAR,
                dma, dma((n_row.bit_length() - 1,)), dma, dma, dma, dma, dma((3,)),
                pltpu.VMEM((2 * cols, rows), BF16),
            ],
            compiler_params=pltpu.CompilerParams(
                collective_id=0, has_side_effects=True,
            ),
        )(boxes, pins[None, :], capacity, cell_bin, cell_area)
        return pl.pallas_call(
            functools.partial(finish, 2.0 / (rows * n_row)),
            out_shape=(
                jax.ShapeDtypeStruct((rows, cols), F32),
                jax.ShapeDtypeStruct((rows, cols), F32),
                jax.ShapeDtypeStruct((1, cells), F32),
            ),
            in_specs=[vmem] * 4,
            out_specs=(hbm,) * 3,
            scratch_shapes=[pltpu.VMEM((rows, cols), F32), dma((3,))],
        )(*[pltpu.with_memory_space_constraint(value, pltpu.VMEM) for value in (rudy, within, size, final)])

    in_specs = (P(None, "col"), P("col"), P("row", "col"), P("row", "col"), P("row", "col"))
    out_specs = (P("row", "col"), P("row", "col"), P("row", "col"))
    return jax.shard_map(
        per_device, mesh=mesh, in_specs=in_specs, out_specs=out_specs, check_vma=False
    )
```

```python
import functools

import jax
import jax.numpy as jnp
from jax import lax
from jax.experimental import pallas as pl
from jax.experimental.pallas import tpu as pltpu
from jax.sharding import PartitionSpec as P

MESH = pl.DeviceIdType.MESH
F32 = jnp.float32
I16 = jnp.int16
F8 = jnp.float8_e4m3fn
BF16 = jnp.bfloat16
NT = (((1,), (1,)), ((), ()))
NN = (((1,), (0,)), ((), ()))


ORDER = ((3, 5, 7, 2, 6, 4), (1, 7, 0, 6, 5, 4), (1, 7, 0, 6, 3, 2), (5, 3, 1, 4, 2, 0))
KNOWN = tuple(max(at for at, slot in enumerate(order) if slot % 2) for order in ORDER)


def split2(value):
    high = value.astype(BF16)
    return high, (value - high.astype(F32)).astype(BF16)


def kernel(
    n_row, n_col,
    boxes_hbm, pins_hbm, cap_hbm, bin_hbm, area_hbm,
    acc, within_ref, size_ref, final_ref,
    boxes_ref, pins_ref, cap_ref, bin_ref, area_ref,
    held_box, held_weight, own_weight, suffix, below_out, below_in, msg, col_out, col_in, looked,
    box_send, weight_send, pass_box, pass_weight, net_recv, token, far_in,
    below_send, below_recv, col_send, col_recv, msg_send, msg_recv, load_sem, table, *units,
):
    sums, looks = units[:2], units[2:]
    rows, cols = acc.shape
    nets = boxes_ref.shape[1]
    cells = bin_ref.shape[1]
    n_chip = n_col // 2
    row = lax.axis_index("row")
    col = lax.axis_index("col")
    chip, core = col // 2, col % 2
    partner = chip * 2 + (1 - core)
    me = row * n_col + col

    both_sides = jnp.minimum(chip, n_chip - 1 - chip)
    longer = jnp.where(chip < n_chip - 1 - chip, 1, -1)

    def nearest(step):
        turn = jnp.where(lax.rem(step, 2) == 1, 1, -1) * ((step + 1) // 2)
        return chip + jnp.where(step <= 2 * both_sides, turn, longer * (step - both_sides))

    reach = min(2, n_chip - 1)
    flips = [1 << bit for bit in range(n_row.bit_length() - 1)]

    def flipped(mask):
        other = row
        for flip in flips:
            if mask & flip:
                other = other + flip * (1 - 2 * (row // flip % 2))
        return other

    def along(offsets, act):
        for offset in offsets:
            target = chip + offset

            @pl.when((target >= 0) & (target < n_chip))
            def _():
                act(target)

    before = range(1 - n_chip, 0)
    after = range(reach, 0, -1)
    beyond = range(n_chip - 1, reach, -1)
    waits_far = chip < n_chip - 1 - reach
    tells_far = (chip > 0) & (chip < n_chip - reach)

    barrier = pltpu.get_barrier_semaphore()

    def greet(target_row, target_col):
        pl.semaphore_signal(barrier, inc=1, device_id=(target_row, target_col), device_id_type=MESH)

    @pl.when(core == 1)
    def _():
        for side in (1, 0):
            along([-offset for offset in (*after, *before)], lambda target: greet(row, target * 2 + side))

    greet(row, partner)
    for flip in flips:
        greet(flipped(flip), col)

    def tell_far(target):
        pl.semaphore_signal(far_in, inc=1, device_id=(row, target), device_id_type=MESH)

    def tell_below():
        tell_far(jnp.maximum(chip - 1, 0) * 2 + 1)

    sources = [(boxes_hbm, boxes_ref, 0), (pins_hbm, pins_ref, 0), (bin_hbm, bin_ref, 1), (area_hbm, area_ref, 1)]
    for source, target, index in (*sources, (cap_hbm, cap_ref, 2)):
        pltpu.make_async_copy(source, target, load_sem.at[index]).start()

    def landed(index, like):
        pltpu.make_async_copy(like, like, load_sem.at[index]).wait()

    net_rows = acc.at[pl.ds(0, 5 * nets // cols)]
    for unit in (*sums, *looks):
        pltpu.matmul_pop(unit)
    landed(0, net_rows)

    span_x = (boxes_ref[1:2, :] - boxes_ref[0:1, :] + 1).astype(F32)
    span_y = (boxes_ref[3:4, :] - boxes_ref[2:3, :] + 1).astype(F32)
    weight = jnp.log(pins_ref[...].astype(F32)) * (span_x + span_y) / (span_x * span_y)
    weight = weight.astype(BF16).astype(F32)
    own_weight[...] = weight
    held_weight[col] = weight
    held_box[col] = boxes_ref[...]

    landed(1, held_weight.at[pl.ds(0, 2)])

    def cell_block(index, size):
        at = pl.ds(index * size, size)
        value = bin_ref[:, at]
        return lax.shift_right_logical(value, cols.bit_length() - 1), value & (cols - 1), area_ref[:, at]

    block = 256
    one, zero = jnp.ones((), BF16), jnp.zeros((), BF16)

    def iota(length, width=block):
        return lax.broadcasted_iota(jnp.int32, (length, width), 0).astype(I16)

    def suffix_sums():
        for index in range(cells // block):
            bin_row, bin_col, area = cell_block(index, block)
            unit, stage = index % 2, index // 2 % 2
            at_or_below = jnp.where(iota(rows) <= bin_row.astype(I16), one, zero)
            high, low = split2(area)
            same = iota(cols) == bin_col.astype(I16)
            held = jnp.concatenate([jnp.where(same, high, zero), jnp.where(same, low, zero)], axis=0)
            pltpu.matmul_push_rhs(held, staging_register=stage, mxu_index=unit, transpose=True)
            pltpu.matmul_acc_lhs(sums[unit], at_or_below, load_staged_rhs=stage)
        total = pltpu.matmul_pop(sums[0]) + pltpu.matmul_pop(sums[1])
        suffix[...] = total[:, :cols] + total[:, cols:]
        below_out[0] = suffix[0:1, :]
        msg[me, 1:2, :] = suffix[0:1, :]

    pl.when(chip < n_chip - 1)(suffix_sums)

    around = chip + jnp.minimum(n_chip - 1 - chip, reach)
    pl.semaphore_wait(barrier, around + 1 + len(flips))
    pl.when((core == 1) & tells_far & jnp.logical_not(waits_far))(tell_below)

    def pair(source, weight_source, slot, target, sends):
        return [
            pltpu.make_async_remote_copy(
                src_ref=src, dst_ref=held.at[slot], send_sem=send, recv_sem=net_recv.at[slot],
                device_id=(row, target), device_id_type=MESH,
            )
            for src, held, send in zip((source, weight_source), (held_box, held_weight), sends)
        ]

    def send_own(target):
        for copy in pair(boxes_ref, own_weight, col, target, (box_send, weight_send)):
            copy.start()

    def send_chip(target):
        send_own(target * 2 + 1)

    along(before, send_chip)
    along(after, send_chip)
    send_own(partner)

    pl.when(chip == n_chip - 1)(suffix_sums)

    def below_copy(bit):
        return pltpu.make_async_remote_copy(
            src_ref=below_out.at[bit], dst_ref=below_in.at[bit], send_sem=below_send,
            recv_sem=below_recv.at[bit], device_id=(flipped(flips[bit]), col), device_id_type=MESH,
        )

    below_copy(0).start()

    @pl.when(waits_far)
    def _():
        pl.semaphore_wait(far_in, 1)
        pl.when(core == 1)(lambda: tell_far(partner))
        along(beyond, send_chip)
        pl.when((core == 1) & tells_far)(tell_below)

    def take_below(bit):
        below_copy(bit).wait_recv()
        if bit + 1 < len(flips):
            below_out[bit + 1] = below_out[bit] + below_in[bit]
            below_copy(bit + 1).start()

    row_start = row * rows
    col_start = col * cols
    one8, zero8 = jnp.ones((rows, block), F8), jnp.zeros((rows, block), F8)
    low_end = jnp.int16(-32768)

    def raster(slot):
        ys, xs = iota(rows) + low_end, iota(cols) + low_end
        for index in range(nets // block):
            at = pl.ds(index * block, block)
            unit, stage = index % 2, index // 2 % 2
            x0, x1 = held_box[slot, 0:1, at], held_box[slot, 1:2, at]
            y0, y1 = held_box[slot, 2:3, at], held_box[slot, 3:4, at]
            scaled = held_weight[slot, :, at] * 16.0
            high = scaled.astype(F8)
            low = ((scaled - high.astype(F32)) * 16.0).astype(F8)
            down = ys - (y0 - row_start).astype(I16) <= (y1 - y0 - 32768).astype(I16)
            across = xs - (x0 - col_start).astype(I16) <= (x1 - x0 - 32768).astype(I16)
            weighted = jnp.concatenate(
                [jnp.where(across, jnp.broadcast_to(part, (cols, block)), zero8[:cols]) for part in (high, low)], axis=0
            )
            pltpu.matmul_push_rhs(weighted, staging_register=stage, mxu_index=unit, transpose=True)
            pltpu.matmul_acc_lhs(sums[unit], jnp.where(down, one8, zero8), load_staged_rhs=stage)

    raster(col)

    def wait_pair(slot):
        pltpu.make_async_remote_copy(
            src_ref=net_rows, dst_ref=net_rows, send_sem=box_send, recv_sem=net_recv.at[slot],
            device_id=(row, partner), device_id_type=MESH,
        ).wait_recv()

    wait_pair(partner)
    raster(partner)

    far_rows = [mask for mask in range(1, n_row) if mask not in flips]

    def scan_rows():
        for bit in range(len(flips) - 1):
            take_below(bit)

    def tell_rows():
        @pl.when(core == 1)
        def _():
            for mask in far_rows:
                pl.semaphore_signal(token, inc=1, device_id=(flipped(mask), col), device_id_type=MESH)

    def take(slot, then=lambda: None):
        wait_pair(slot)

        @pl.when(core == 1)
        def _():
            for copy in pair(held_box.at[slot], held_weight.at[slot], slot, partner, (pass_box, pass_weight)):
                copy.start()

        then()
        raster(slot)

    late = chip == n_chip - 1
    pl.when(jnp.logical_not(late))(scan_rows)
    if n_chip == len(ORDER):
        for step in range(n_col - 2):
            slot = sum(jnp.where(chip == at, ORDER[at][step], 0) for at in range(n_chip))
            known = sum(jnp.where(chip == at, KNOWN[at] == step, False) for at in range(n_chip)) > 0
            take(slot, (lambda: pl.when(known)(tell_rows)) if step in KNOWN else lambda: None)
            if step == 0:
                pl.when(late)(scan_rows)
    else:
        for side in (1, 0):
            lax.fori_loop(1, n_chip, lambda step, carry: (take(nearest(step) * 2 + side), carry)[1], 0)
            if side:
                pl.when(late)(scan_rows)
                tell_rows()
    take_below(len(flips) - 1)
    below = jnp.zeros((1, cols), F32)
    for bit, flip in enumerate(flips):
        below += jnp.where(row // flip % 2 == 0, below_in[bit], jnp.zeros((), F32))

    @pl.when(core == 1)
    def _():
        pl.semaphore_wait(token, len(far_rows))
        pl.semaphore_signal(token, inc=1, device_id=(row, partner), device_id_type=MESH)

    @pl.when(core == 0)
    def _():
        pl.semaphore_wait(token, 1)

    landed(2, cap_ref)
    both = pltpu.matmul_pop(sums[0]) + pltpu.matmul_pop(sums[1])
    acc[...] = both[:, :cols] * (1.0 / 16.0) + both[:, cols:] * (1.0 / 256.0)
    excess = jnp.maximum(acc[...] - cap_ref[...], 0.0)
    col_out[...] = jnp.sum(excess, axis=0, keepdims=True)
    growth = jnp.sum(excess * (suffix[...] + below), axis=0, keepdims=True)
    msg[me, 0:1, :] = growth

    def column_copy(offset):
        target = lax.rem(row + offset, n_row)
        return pltpu.make_async_remote_copy(
            src_ref=col_out, dst_ref=col_in.at[row], send_sem=col_send, recv_sem=col_recv,
            device_id=(target, col), device_id_type=MESH,
        )

    for offset in range(1, n_row):
        column_copy(offset).start()

    def message(mask, step, side):
        target = (nearest(step) if step else chip) * 2 + (core if side else 1 - core)
        return pltpu.make_async_remote_copy(
            src_ref=msg.at[me], dst_ref=msg.at[me], send_sem=msg_send, recv_sem=msg_recv,
            device_id=(flipped(mask), target), device_id_type=MESH,
        )

    def hops(at):
        mask, step, _ = at
        return -(mask.bit_count() + step)

    everyone = [(mask, step, side) for mask in range(n_row) for step in range(n_chip) for side in (0, 1)]
    for at in sorted(everyone, key=hops):
        if at != (0, 0, 1):
            message(*at).start()

    parts = jnp.concatenate(split2(excess), axis=1)
    for index in range(rows // block):
        unit, stage = index % 2, index // 2 % 2
        above = lax.broadcasted_iota(jnp.int32, (rows, block), 1).astype(I16) + jnp.int16(index * block)
        lower = jnp.where(iota(rows) >= above, one, zero)
        pltpu.matmul_push_rhs(parts[index * block:(index + 1) * block], staging_register=stage, mxu_index=unit)
        pltpu.matmul_acc_lhs(sums[unit], lower, load_staged_rhs=stage)
    both = pltpu.matmul_pop(sums[0]) + pltpu.matmul_pop(sums[1])
    within = both[:, :cols] + both[:, cols:]
    within_ref[...] = within
    table[...] = jnp.concatenate(split2(within.T), axis=0)
    columns = lax.broadcasted_iota(jnp.int32, (cols, block), 0)
    for index in range(cells // block):
        bin_row, bin_col, _ = cell_block(index, block)
        unit = index % 2
        got = looks[index % len(looks)]
        for part in range(rows // block):
            at = pl.ds(part * block, block)
            same = jnp.where(iota(block) == (bin_row - part * block).astype(I16), one, zero)
            pltpu.matmul_push_rhs(same, staging_register=part % 2, mxu_index=unit)
            pltpu.matmul_acc_lhs(got, table[:, at], load_staged_rhs=part % 2)
        got = pltpu.matmul_pop(got)
        got = jnp.where(columns == bin_col, got[:cols] + got[cols:], 0.0)
        looked[:, pl.ds(index * block, block)] = jnp.sum(got, axis=0, keepdims=True)

    def drain(like, send, recv=None):
        copy = pltpu.make_async_remote_copy(
            src_ref=like, dst_ref=like, send_sem=send, recv_sem=col_recv if recv is None else recv,
            device_id=(row, partner), device_id_type=MESH,
        )
        copy.wait_send()
        if recv is not None:
            copy.wait_recv()

    drain(held_box.at[pl.ds(0, n_chip)], box_send)
    drain(held_weight.at[pl.ds(0, n_chip)], weight_send)

    @pl.when(core == 1)
    def _():
        drain(held_box.at[pl.ds(0, n_col - 2)], pass_box)
        drain(held_weight.at[pl.ds(0, n_col - 2)], pass_weight)

    drain(below_out.at[pl.ds(0, len(flips))], below_send)
    drain(col_in.at[pl.ds(0, n_row - 1)], col_send, col_recv)
    carried = jnp.zeros((1, cols), F32)
    for index in range(n_row):
        carried += jnp.where(index < row, col_in[index], jnp.zeros((), F32))
    scale = 2.0 / (rows * n_row)
    turned_carry = jnp.broadcast_to(carried, (8, cols)).T[:, 0:1]
    for index in range(cells // block):
        at = pl.ds(index * block, block)
        _, bin_col, area = cell_block(index, block)
        got = jnp.where(columns == bin_col, turned_carry, 0.0)
        got = looked[:, at] + jnp.sum(got, axis=0, keepdims=True)
        looked[:, at] = area * (1.0 + scale * got)
    final_ref[...] = jnp.broadcast_to(1.0 + scale * carried, final_ref.shape)

    drain(msg.at[pl.ds(0, n_row * n_col - 1)], msg_send, msg_recv)
    sums_all = jnp.sum(jnp.sum(msg[...], axis=0), axis=1, keepdims=True)
    growth_total, area_total = sums_all[0:1], sums_all[1:2]
    size_ref[...] = looked[...] * (area_total / (area_total + scale * growth_total))


def with_units(body, *refs):
    rows, cols = refs[5].shape
    wide = 2 * cols
    pl.run_scoped(
        functools.partial(body, *refs),
        *[pltpu.ACC(unit)((rows, wide), F32) for unit in (0, 1)],
        *[pltpu.ACC(unit)((wide, wide), F32) for unit in (0, 1, 0, 1)],
    )


def finish(scale, rudy, within, size, final, rudy_hbm, infl_hbm, size_hbm, infl, sems):
    first = pltpu.make_async_copy(rudy, rudy_hbm, sems.at[0])
    second = pltpu.make_async_copy(size, size_hbm, sems.at[1])
    third = pltpu.make_async_copy(infl, infl_hbm, sems.at[2])
    first.start()
    second.start()
    infl[...] = final[0:1, :] + scale * within[...]
    third.start()
    first.wait()
    second.wait()
    third.wait()


def solution(mesh):
    n_row, n_col = mesh.shape["row"], mesh.shape["col"]

    def per_device(boxes, pins, capacity, cell_bin, cell_area):
        rows, cols = capacity.shape
        nets = boxes.shape[1]
        cells = cell_bin.shape[1]
        vmem = pl.BlockSpec(memory_space=pltpu.VMEM)
        hbm = pl.BlockSpec(memory_space=pl.ANY)
        dma = pltpu.SemaphoreType.DMA
        rudy, within, size, final = pl.pallas_call(
            functools.partial(with_units, functools.partial(kernel, n_row, n_col)),
            out_shape=(
                pltpu.VMEM((rows, cols), F32),
                pltpu.VMEM((rows, cols), F32),
                pltpu.VMEM((1, cells), F32),
                pltpu.VMEM((8, cols), F32),
            ),
            in_specs=[hbm] * 5,
            out_specs=(vmem,) * 4,
            scratch_shapes=[
                pltpu.VMEM((4, nets), jnp.int32),
                pltpu.VMEM((1, nets), jnp.int32),
                pltpu.VMEM((rows, cols), F32),
                pltpu.VMEM((1, cells), jnp.int32),
                pltpu.VMEM((1, cells), F32),
                pltpu.VMEM((n_col, 4, nets), jnp.int32),
                pltpu.VMEM((n_col, 1, nets), F32),
                pltpu.VMEM((1, nets), F32),
                pltpu.VMEM((rows, cols), F32),
                pltpu.VMEM((n_row, 1, cols), F32),
                pltpu.VMEM((n_row, 1, cols), F32),
                pltpu.VMEM((n_row * n_col, 2, cols), F32),
                pltpu.VMEM((1, cols), F32),
                pltpu.VMEM((n_row, 1, cols), F32),
                pltpu.VMEM((1, cells), F32),
                dma, dma, dma, dma, dma((n_col,)), pltpu.SemaphoreType.REGULAR, pltpu.SemaphoreType.REGULAR,
                dma, dma((n_row.bit_length() - 1,)), dma, dma, dma, dma, dma((3,)),
                pltpu.VMEM((2 * cols, rows), BF16),
            ],
            compiler_params=pltpu.CompilerParams(
                collective_id=0, has_side_effects=True,
            ),
        )(boxes, pins[None, :], capacity, cell_bin, cell_area)
        return pl.pallas_call(
            functools.partial(finish, 2.0 / (rows * n_row)),
            out_shape=(
                jax.ShapeDtypeStruct((rows, cols), F32),
                jax.ShapeDtypeStruct((rows, cols), F32),
                jax.ShapeDtypeStruct((1, cells), F32),
            ),
            in_specs=[vmem] * 4,
            out_specs=(hbm,) * 3,
            scratch_shapes=[pltpu.VMEM((rows, cols), F32), dma((3,))],
        )(*[pltpu.with_memory_space_constraint(value, pltpu.VMEM) for value in (rudy, within, size, final)])

    in_specs = (P(None, "col"), P("col"), P("row", "col"), P("row", "col"), P("row", "col"))
    out_specs = (P("row", "col"), P("row", "col"), P("row", "col"))
    return jax.shard_map(
        per_device, mesh=mesh, in_specs=in_specs, out_specs=out_specs, check_vma=False
    )
```

```python
import functools

import jax
import jax.numpy as jnp
from jax import lax
from jax.experimental import pallas as pl
from jax.experimental.pallas import tpu as pltpu
from jax.sharding import PartitionSpec as P

MESH = pl.DeviceIdType.MESH
F32 = jnp.float32
I16 = jnp.int16
F8 = jnp.float8_e4m3fn
BF16 = jnp.bfloat16
NT = (((1,), (1,)), ((), ()))
NN = (((1,), (0,)), ((), ()))


ORDER = ((3, 5, 7, 2, 6, 4), (1, 7, 0, 6, 5, 4), (1, 7, 0, 6, 3, 2), (5, 3, 1, 4, 2, 0))
KNOWN = tuple(max(at for at, slot in enumerate(order) if slot % 2) for order in ORDER)


def split2(value):
    high = value.astype(BF16)
    return high, (value - high.astype(F32)).astype(BF16)


def kernel(
    n_row, n_col,
    boxes_hbm, pins_hbm, cap_hbm, bin_hbm, area_hbm,
    acc, within_ref, size_ref, final_ref,
    boxes_ref, pins_ref, cap_ref, bin_ref, area_ref,
    held_box, held_weight, own_weight, suffix, below_out, below_in, msg, col_out, col_in, looked,
    box_send, weight_send, pass_box, pass_weight, net_recv, token, far_in,
    below_send, below_recv, col_send, col_recv, msg_send, msg_recv, load_sem, table, *units,
):
    sums, looks = units[:2], units[2:]
    rows, cols = acc.shape
    nets = boxes_ref.shape[1]
    cells = bin_ref.shape[1]
    n_chip = n_col // 2
    row = lax.axis_index("row")
    col = lax.axis_index("col")
    chip, core = col // 2, col % 2
    partner = chip * 2 + (1 - core)
    me = row * n_col + col

    both_sides = jnp.minimum(chip, n_chip - 1 - chip)
    longer = jnp.where(chip < n_chip - 1 - chip, 1, -1)

    def nearest(step):
        turn = jnp.where(lax.rem(step, 2) == 1, 1, -1) * ((step + 1) // 2)
        return chip + jnp.where(step <= 2 * both_sides, turn, longer * (step - both_sides))

    reach = min(2, n_chip - 1)
    flips = [1 << bit for bit in range(n_row.bit_length() - 1)]

    def flipped(mask):
        other = row
        for flip in flips:
            if mask & flip:
                other = other + flip * (1 - 2 * (row // flip % 2))
        return other

    sources = [(boxes_hbm, boxes_ref, 0), (pins_hbm, pins_ref, 0), (bin_hbm, bin_ref, 1), (area_hbm, area_ref, 1)]
    for source, target, index in (*sources, (cap_hbm, cap_ref, 2)):
        pltpu.make_async_copy(source, target, load_sem.at[index]).start()

    def along(offsets, act):
        for offset in offsets:
            target = chip + offset

            @pl.when((target >= 0) & (target < n_chip))
            def _():
                act(target)

    before = range(1 - n_chip, 0)
    after = range(reach, 0, -1)
    beyond = range(n_chip - 1, reach, -1)
    waits_far = chip < n_chip - 1 - reach
    tells_far = (chip > 0) & (chip < n_chip - reach)

    barrier = pltpu.get_barrier_semaphore()

    def greet(target_row, target_col):
        pl.semaphore_signal(barrier, inc=1, device_id=(target_row, target_col), device_id_type=MESH)

    @pl.when(core == 1)
    def _():
        for side in (1, 0):
            along([-offset for offset in (*after, *before)], lambda target: greet(row, target * 2 + side))

    greet(row, partner)
    for flip in flips:
        greet(flipped(flip), col)

    def tell_far(target):
        pl.semaphore_signal(far_in, inc=1, device_id=(row, target), device_id_type=MESH)

    def tell_below():
        tell_far(jnp.maximum(chip - 1, 0) * 2 + 1)

    def landed(index, like):
        pltpu.make_async_copy(like, like, load_sem.at[index]).wait()

    net_rows = acc.at[pl.ds(0, 5 * nets // cols)]
    for unit in (*sums, *looks):
        pltpu.matmul_pop(unit)
    landed(0, net_rows)

    span_x = (boxes_ref[1:2, :] - boxes_ref[0:1, :] + 1).astype(F32)
    span_y = (boxes_ref[3:4, :] - boxes_ref[2:3, :] + 1).astype(F32)
    weight = jnp.log(pins_ref[...].astype(F32)) * (span_x + span_y) / (span_x * span_y)
    weight = weight.astype(BF16).astype(F32)
    own_weight[...] = weight
    held_weight[col] = weight
    held_box[col] = boxes_ref[...]

    landed(1, held_weight.at[pl.ds(0, 2)])

    def cell_block(index, size):
        at = pl.ds(index * size, size)
        value = bin_ref[:, at]
        return lax.shift_right_logical(value, cols.bit_length() - 1), value & (cols - 1), area_ref[:, at]

    block = 256
    one, zero = jnp.ones((), BF16), jnp.zeros((), BF16)

    def iota(length, width=block):
        return lax.broadcasted_iota(jnp.int32, (length, width), 0).astype(I16)

    def suffix_sums():
        for index in range(cells // block):
            bin_row, bin_col, area = cell_block(index, block)
            unit, stage = index % 2, index // 2 % 2
            at_or_below = jnp.where(iota(rows) <= bin_row.astype(I16), one, zero)
            high, low = split2(area)
            same = iota(cols) == bin_col.astype(I16)
            held = jnp.concatenate([jnp.where(same, high, zero), jnp.where(same, low, zero)], axis=0)
            pltpu.matmul_push_rhs(held, staging_register=stage, mxu_index=unit, transpose=True)
            pltpu.matmul_acc_lhs(sums[unit], at_or_below, load_staged_rhs=stage)
        total = pltpu.matmul_pop(sums[0]) + pltpu.matmul_pop(sums[1])
        suffix[...] = total[:, :cols] + total[:, cols:]
        below_out[0] = suffix[0:1, :]
        msg[me, 1:2, :] = suffix[0:1, :]

    pl.when(chip < n_chip - 1)(suffix_sums)

    around = chip + jnp.minimum(n_chip - 1 - chip, reach)
    pl.semaphore_wait(barrier, around + 1 + len(flips))
    pl.when((core == 1) & tells_far & jnp.logical_not(waits_far))(tell_below)

    def pair(source, weight_source, slot, target, sends):
        return [
            pltpu.make_async_remote_copy(
                src_ref=src, dst_ref=held.at[slot], send_sem=send, recv_sem=net_recv.at[slot],
                device_id=(row, target), device_id_type=MESH,
            )
            for src, held, send in zip((source, weight_source), (held_box, held_weight), sends)
        ]

    def send_own(target):
        for copy in pair(boxes_ref, own_weight, col, target, (box_send, weight_send)):
            copy.start()

    def send_chip(target):
        send_own(target * 2 + 1)

    along(before, send_chip)
    along(after, send_chip)
    send_own(partner)

    pl.when(chip == n_chip - 1)(suffix_sums)

    def below_copy(bit):
        return pltpu.make_async_remote_copy(
            src_ref=below_out.at[bit], dst_ref=below_in.at[bit], send_sem=below_send,
            recv_sem=below_recv.at[bit], device_id=(flipped(flips[bit]), col), device_id_type=MESH,
        )

    below_copy(0).start()

    @pl.when(waits_far)
    def _():
        pl.semaphore_wait(far_in, 1)
        pl.when(core == 1)(lambda: tell_far(partner))
        along(beyond, send_chip)
        pl.when((core == 1) & tells_far)(tell_below)

    def take_below(bit):
        below_copy(bit).wait_recv()
        if bit + 1 < len(flips):
            below_out[bit + 1] = below_out[bit] + below_in[bit]
            below_copy(bit + 1).start()

    row_start = row * rows
    col_start = col * cols
    one8, zero8 = jnp.ones((rows, block), F8), jnp.zeros((rows, block), F8)
    low_end = jnp.int16(-32768)

    def raster(slot):
        ys, xs = iota(rows) + low_end, iota(cols) + low_end
        for index in range(nets // block):
            at = pl.ds(index * block, block)
            unit, stage = index % 2, index // 2 % 2
            x0, x1 = held_box[slot, 0:1, at], held_box[slot, 1:2, at]
            y0, y1 = held_box[slot, 2:3, at], held_box[slot, 3:4, at]
            scaled = held_weight[slot, :, at] * 16.0
            high = scaled.astype(F8)
            low = ((scaled - high.astype(F32)) * 16.0).astype(F8)
            down = ys - (y0 - row_start).astype(I16) <= (y1 - y0 - 32768).astype(I16)
            across = xs - (x0 - col_start).astype(I16) <= (x1 - x0 - 32768).astype(I16)
            weighted = jnp.concatenate(
                [jnp.where(across, jnp.broadcast_to(part, (cols, block)), zero8[:cols]) for part in (high, low)], axis=0
            )
            pltpu.matmul_push_rhs(weighted, staging_register=stage, mxu_index=unit, transpose=True)
            pltpu.matmul_acc_lhs(sums[unit], jnp.where(down, one8, zero8), load_staged_rhs=stage)

    def wait_pair(slot):
        pltpu.make_async_remote_copy(
            src_ref=net_rows, dst_ref=net_rows, send_sem=box_send, recv_sem=net_recv.at[slot],
            device_id=(row, partner), device_id_type=MESH,
        ).wait_recv()


    far_rows = [mask for mask in range(1, n_row) if mask not in flips]

    def scan_rows():
        for bit in range(len(flips) - 1):
            take_below(bit)

    def tell_rows():
        for mask in far_rows:
            pl.semaphore_signal(token, inc=1, device_id=(flipped(mask), col), device_id_type=MESH)

    def take(slot, ready, then=lambda: None):
        @pl.when(core == 1)
        def _():
            wait_pair(slot)
            for copy in pair(held_box.at[slot], held_weight.at[slot], slot, partner, (pass_box, pass_weight)):
                copy.start()
            then()

        raster(ready)

        @pl.when(core == 0)
        def _():
            wait_pair(slot)

    raster(col)
    wait_pair(partner)
    ready = partner
    late = chip == n_chip - 1
    pl.when(jnp.logical_not(late))(scan_rows)
    if n_chip == len(ORDER):
        for step in range(n_col - 2):
            slot = sum(jnp.where(chip == at, ORDER[at][step], 0) for at in range(n_chip))
            known = sum(jnp.where(chip == at, KNOWN[at] == step, False) for at in range(n_chip)) > 0
            take(slot, ready, (lambda: pl.when(known)(tell_rows)) if step in KNOWN else lambda: None)
            ready = slot
            if step == 0:
                pl.when(late)(scan_rows)
    else:
        for side in (1, 0):
            def step(index, ready):
                slot = nearest(index) * 2 + side
                take(slot, ready)
                return slot

            ready = lax.fori_loop(1, n_chip, step, ready)
            if side:
                pl.when(late)(scan_rows)
                pl.when(core == 1)(tell_rows)
    raster(ready)
    take_below(len(flips) - 1)
    below = jnp.zeros((1, cols), F32)
    for bit, flip in enumerate(flips):
        below += jnp.where(row // flip % 2 == 0, below_in[bit], jnp.zeros((), F32))

    @pl.when(core == 1)
    def _():
        pl.semaphore_wait(token, len(far_rows))
        pl.semaphore_signal(token, inc=1, device_id=(row, partner), device_id_type=MESH)

    @pl.when(core == 0)
    def _():
        pl.semaphore_wait(token, 1)

    landed(2, cap_ref)
    both = pltpu.matmul_pop(sums[0]) + pltpu.matmul_pop(sums[1])
    acc[...] = both[:, :cols] * (1.0 / 16.0) + both[:, cols:] * (1.0 / 256.0)
    excess = jnp.maximum(acc[...] - cap_ref[...], 0.0)
    col_out[...] = jnp.sum(excess, axis=0, keepdims=True)
    growth = jnp.sum(excess * (suffix[...] + below), axis=0, keepdims=True)
    msg[me, 0:1, :] = growth

    def column_copy(offset):
        target = lax.rem(row + offset, n_row)
        return pltpu.make_async_remote_copy(
            src_ref=col_out, dst_ref=col_in.at[row], send_sem=col_send, recv_sem=col_recv,
            device_id=(target, col), device_id_type=MESH,
        )

    for offset in range(1, n_row):
        column_copy(offset).start()

    def message(mask, step, side):
        target = (nearest(step) if step else chip) * 2 + (core if side else 1 - core)
        return pltpu.make_async_remote_copy(
            src_ref=msg.at[me], dst_ref=msg.at[me], send_sem=msg_send, recv_sem=msg_recv,
            device_id=(flipped(mask), target), device_id_type=MESH,
        )

    def hops(at):
        mask, step, _ = at
        return -(mask.bit_count() + step)

    everyone = [(mask, step, side) for mask in range(n_row) for step in range(n_chip) for side in (0, 1)]
    for at in sorted(everyone, key=hops):
        if at != (0, 0, 1):
            message(*at).start()

    parts = jnp.concatenate(split2(excess), axis=1)
    for index in range(rows // block):
        unit, stage = index % 2, index // 2 % 2
        above = lax.broadcasted_iota(jnp.int32, (rows, block), 1).astype(I16) + jnp.int16(index * block)
        lower = jnp.where(iota(rows) >= above, one, zero)
        pltpu.matmul_push_rhs(parts[index * block:(index + 1) * block], staging_register=stage, mxu_index=unit)
        pltpu.matmul_acc_lhs(sums[unit], lower, load_staged_rhs=stage)
    both = pltpu.matmul_pop(sums[0]) + pltpu.matmul_pop(sums[1])
    within = both[:, :cols] + both[:, cols:]
    within_ref[...] = within
    table[...] = jnp.concatenate(split2(within.T), axis=0)
    columns = lax.broadcasted_iota(jnp.int32, (cols, block), 0)
    for index in range(cells // block):
        bin_row, bin_col, _ = cell_block(index, block)
        unit = index % 2
        got = looks[index % len(looks)]
        for part in range(rows // block):
            at = pl.ds(part * block, block)
            same = jnp.where(iota(block) == (bin_row - part * block).astype(I16), one, zero)
            pltpu.matmul_push_rhs(same, staging_register=part % 2, mxu_index=unit)
            pltpu.matmul_acc_lhs(got, table[:, at], load_staged_rhs=part % 2)
        got = pltpu.matmul_pop(got)
        got = jnp.where(columns == bin_col, got[:cols] + got[cols:], 0.0)
        looked[:, pl.ds(index * block, block)] = jnp.sum(got, axis=0, keepdims=True)

    def drain(like, send, recv=None):
        copy = pltpu.make_async_remote_copy(
            src_ref=like, dst_ref=like, send_sem=send, recv_sem=col_recv if recv is None else recv,
            device_id=(row, partner), device_id_type=MESH,
        )
        copy.wait_send()
        if recv is not None:
            copy.wait_recv()

    drain(held_box.at[pl.ds(0, n_chip)], box_send)
    drain(held_weight.at[pl.ds(0, n_chip)], weight_send)

    @pl.when(core == 1)
    def _():
        drain(held_box.at[pl.ds(0, n_col - 2)], pass_box)
        drain(held_weight.at[pl.ds(0, n_col - 2)], pass_weight)

    drain(below_out.at[pl.ds(0, len(flips))], below_send)
    drain(col_in.at[pl.ds(0, n_row - 1)], col_send, col_recv)
    carried = jnp.zeros((1, cols), F32)
    for index in range(n_row):
        carried += jnp.where(index < row, col_in[index], jnp.zeros((), F32))
    scale = 2.0 / (rows * n_row)
    turned_carry = jnp.broadcast_to(carried, (8, cols)).T[:, 0:1]
    for index in range(cells // block):
        at = pl.ds(index * block, block)
        _, bin_col, area = cell_block(index, block)
        got = jnp.where(columns == bin_col, turned_carry, 0.0)
        got = looked[:, at] + jnp.sum(got, axis=0, keepdims=True)
        looked[:, at] = area * (1.0 + scale * got)
    final_ref[...] = jnp.broadcast_to(1.0 + scale * carried, final_ref.shape)

    drain(msg.at[pl.ds(0, n_row * n_col - 1)], msg_send, msg_recv)
    sums_all = jnp.sum(jnp.sum(msg[...], axis=0), axis=1, keepdims=True)
    growth_total, area_total = sums_all[0:1], sums_all[1:2]
    size_ref[...] = looked[...] * (area_total / (area_total + scale * growth_total))


def with_units(body, *refs):
    rows, cols = refs[5].shape
    wide = 2 * cols
    pl.run_scoped(
        functools.partial(body, *refs),
        *[pltpu.ACC(unit)((rows, wide), F32) for unit in (0, 1)],
        *[pltpu.ACC(unit)((wide, wide), F32) for unit in (0, 1, 0, 1)],
    )


def finish(scale, rudy, within, size, final, rudy_hbm, infl_hbm, size_hbm, infl, sems):
    first = pltpu.make_async_copy(rudy, rudy_hbm, sems.at[0])
    second = pltpu.make_async_copy(size, size_hbm, sems.at[1])
    third = pltpu.make_async_copy(infl, infl_hbm, sems.at[2])
    first.start()
    second.start()
    infl[...] = final[0:1, :] + scale * within[...]
    third.start()
    first.wait()
    second.wait()
    third.wait()


def solution(mesh):
    n_row, n_col = mesh.shape["row"], mesh.shape["col"]

    def per_device(boxes, pins, capacity, cell_bin, cell_area):
        rows, cols = capacity.shape
        nets = boxes.shape[1]
        cells = cell_bin.shape[1]
        vmem = pl.BlockSpec(memory_space=pltpu.VMEM)
        hbm = pl.BlockSpec(memory_space=pl.ANY)
        dma = pltpu.SemaphoreType.DMA
        rudy, within, size, final = pl.pallas_call(
            functools.partial(with_units, functools.partial(kernel, n_row, n_col)),
            out_shape=(
                pltpu.VMEM((rows, cols), F32),
                pltpu.VMEM((rows, cols), F32),
                pltpu.VMEM((1, cells), F32),
                pltpu.VMEM((8, cols), F32),
            ),
            in_specs=[hbm] * 5,
            out_specs=(vmem,) * 4,
            scratch_shapes=[
                pltpu.VMEM((4, nets), jnp.int32),
                pltpu.VMEM((1, nets), jnp.int32),
                pltpu.VMEM((rows, cols), F32),
                pltpu.VMEM((1, cells), jnp.int32),
                pltpu.VMEM((1, cells), F32),
                pltpu.VMEM((n_col, 4, nets), jnp.int32),
                pltpu.VMEM((n_col, 1, nets), F32),
                pltpu.VMEM((1, nets), F32),
                pltpu.VMEM((rows, cols), F32),
                pltpu.VMEM((n_row, 1, cols), F32),
                pltpu.VMEM((n_row, 1, cols), F32),
                pltpu.VMEM((n_row * n_col, 2, cols), F32),
                pltpu.VMEM((1, cols), F32),
                pltpu.VMEM((n_row, 1, cols), F32),
                pltpu.VMEM((1, cells), F32),
                dma, dma, dma, dma, dma((n_col,)), pltpu.SemaphoreType.REGULAR, pltpu.SemaphoreType.REGULAR,
                dma, dma((n_row.bit_length() - 1,)), dma, dma, dma, dma, dma((3,)),
                pltpu.VMEM((2 * cols, rows), BF16),
            ],
            compiler_params=pltpu.CompilerParams(
                collective_id=0, has_side_effects=True,
            ),
        )(boxes, pins[None, :], capacity, cell_bin, cell_area)
        return pl.pallas_call(
            functools.partial(finish, 2.0 / (rows * n_row)),
            out_shape=(
                jax.ShapeDtypeStruct((rows, cols), F32),
                jax.ShapeDtypeStruct((rows, cols), F32),
                jax.ShapeDtypeStruct((1, cells), F32),
            ),
            in_specs=[vmem] * 4,
            out_specs=(hbm,) * 3,
            scratch_shapes=[pltpu.VMEM((rows, cols), F32), dma((3,))],
        )(*[pltpu.with_memory_space_constraint(value, pltpu.VMEM) for value in (rudy, within, size, final)])

    in_specs = (P(None, "col"), P("col"), P("row", "col"), P("row", "col"), P("row", "col"))
    out_specs = (P("row", "col"), P("row", "col"), P("row", "col"))
    return jax.shard_map(
        per_device, mesh=mesh, in_specs=in_specs, out_specs=out_specs, check_vma=False
    )
```

```python
import functools

import jax
import jax.numpy as jnp
from jax import lax
from jax.experimental import pallas as pl
from jax.experimental.pallas import tpu as pltpu
from jax.sharding import PartitionSpec as P

MESH = pl.DeviceIdType.MESH
F32 = jnp.float32
I16 = jnp.int16
F8 = jnp.float8_e4m3fn
BF16 = jnp.bfloat16
NT = (((1,), (1,)), ((), ()))
NN = (((1,), (0,)), ((), ()))


ORDER = ((3, 5, 7, 2, 6, 4), (1, 7, 0, 6, 5, 4), (1, 7, 0, 6, 3, 2), (5, 3, 1, 2, 0, 4))
LATE = (5, 4, 3, 1, 2, 0)
KNOWN = tuple(max(at for at, slot in enumerate(order) if slot % 2) for order in ORDER)


def split2(value):
    high = value.astype(BF16)
    return high, (value - high.astype(F32)).astype(BF16)


def kernel(
    n_row, n_col,
    boxes_hbm, pins_hbm, cap_hbm, bin_hbm, area_hbm,
    acc, within_ref, size_ref, final_ref,
    boxes_ref, pins_ref, cap_ref, bin_ref, area_ref,
    held_box, held_weight, own_weight, suffix, below_out, below_in, msg, col_out, col_in, looked,
    box_send, weight_send, pass_box, pass_weight, net_recv, token, far_in,
    below_send, below_recv, col_send, col_recv, msg_send, msg_recv, load_sem, table, *units,
):
    sums, looks = units[:2], units[2:]
    rows, cols = acc.shape
    nets = boxes_ref.shape[1]
    cells = bin_ref.shape[1]
    n_chip = n_col // 2
    row = lax.axis_index("row")
    col = lax.axis_index("col")
    chip, core = col // 2, col % 2
    partner = chip * 2 + (1 - core)
    me = row * n_col + col

    both_sides = jnp.minimum(chip, n_chip - 1 - chip)
    longer = jnp.where(chip < n_chip - 1 - chip, 1, -1)

    def nearest(step):
        turn = jnp.where(lax.rem(step, 2) == 1, 1, -1) * ((step + 1) // 2)
        return chip + jnp.where(step <= 2 * both_sides, turn, longer * (step - both_sides))

    reach = min(2, n_chip - 1)
    flips = [1 << bit for bit in range(n_row.bit_length() - 1)]

    def flipped(mask):
        other = row
        for flip in flips:
            if mask & flip:
                other = other + flip * (1 - 2 * (row // flip % 2))
        return other

    sources = [(boxes_hbm, boxes_ref, 0), (pins_hbm, pins_ref, 0), (bin_hbm, bin_ref, 1), (area_hbm, area_ref, 1)]
    for source, target, index in (*sources, (cap_hbm, cap_ref, 2)):
        pltpu.make_async_copy(source, target, load_sem.at[index]).start()

    def along(offsets, act):
        for offset in offsets:
            target = chip + offset

            @pl.when((target >= 0) & (target < n_chip))
            def _():
                act(target)

    before = range(1 - n_chip, 0)
    after = range(reach, 0, -1)
    beyond = range(n_chip - 1, reach, -1)
    late = chip == n_chip - 1
    before_late = (core == 0) & (chip == n_chip - 2)
    waits_far = chip < n_chip - 1 - reach
    tells_far = (chip > 0) & (chip < n_chip - reach)

    barrier = pltpu.get_barrier_semaphore()

    def greet(target_row, target_col):
        pl.semaphore_signal(barrier, inc=1, device_id=(target_row, target_col), device_id_type=MESH)

    @pl.when(core == 1)
    def _():
        for side in (1, 0):
            along([-offset for offset in (*after, *before)], lambda target: greet(row, target * 2 + side))

    @pl.when((core == 0) & late)
    def _():
        greet(row, col - 2)

    greet(row, partner)
    for flip in flips:
        greet(flipped(flip), col)

    def tell_far(target):
        pl.semaphore_signal(far_in, inc=1, device_id=(row, target), device_id_type=MESH)

    def tell_below():
        tell_far(jnp.maximum(chip - 1, 0) * 2 + 1)

    def landed(index, like):
        pltpu.make_async_copy(like, like, load_sem.at[index]).wait()

    net_rows = acc.at[pl.ds(0, 5 * nets // cols)]
    for unit in (*sums, *looks):
        pltpu.matmul_pop(unit)
    landed(0, net_rows)

    span_x = (boxes_ref[1:2, :] - boxes_ref[0:1, :] + 1).astype(F32)
    span_y = (boxes_ref[3:4, :] - boxes_ref[2:3, :] + 1).astype(F32)
    weight = jnp.log(pins_ref[...].astype(F32)) * (span_x + span_y) / (span_x * span_y)
    weight = weight.astype(BF16).astype(F32)
    own_weight[...] = weight
    held_weight[col] = weight
    held_box[col] = boxes_ref[...]

    landed(1, held_weight.at[pl.ds(0, 2)])

    def cell_block(index, size):
        at = pl.ds(index * size, size)
        value = bin_ref[:, at]
        return lax.shift_right_logical(value, cols.bit_length() - 1), value & (cols - 1), area_ref[:, at]

    block = 256
    one, zero = jnp.ones((), BF16), jnp.zeros((), BF16)

    def iota(length, width=block):
        return lax.broadcasted_iota(jnp.int32, (length, width), 0).astype(I16)

    def suffix_sums():
        for index in range(cells // block):
            bin_row, bin_col, area = cell_block(index, block)
            unit, stage = index % 2, index // 2 % 2
            at_or_below = jnp.where(iota(rows) <= bin_row.astype(I16), one, zero)
            high, low = split2(area)
            same = iota(cols) == bin_col.astype(I16)
            held = jnp.concatenate([jnp.where(same, high, zero), jnp.where(same, low, zero)], axis=0)
            pltpu.matmul_push_rhs(held, staging_register=stage, mxu_index=unit, transpose=True)
            pltpu.matmul_acc_lhs(sums[unit], at_or_below, load_staged_rhs=stage)
        total = pltpu.matmul_pop(sums[0]) + pltpu.matmul_pop(sums[1])
        suffix[...] = total[:, :cols] + total[:, cols:]
        below_out[0] = suffix[0:1, :]
        msg[me, 1:2, :] = suffix[0:1, :]

    pl.when(chip < n_chip - 1)(suffix_sums)

    around = chip + jnp.minimum(n_chip - 1 - chip, reach)
    pl.semaphore_wait(barrier, around + 1 + len(flips) + jnp.where(before_late, 1, 0))
    pl.when((core == 1) & tells_far & jnp.logical_not(waits_far))(tell_below)

    def pair(source, weight_source, slot, target, sends):
        return [
            pltpu.make_async_remote_copy(
                src_ref=src, dst_ref=held.at[slot], send_sem=send, recv_sem=net_recv.at[slot],
                device_id=(row, target), device_id_type=MESH,
            )
            for src, held, send in zip((source, weight_source), (held_box, held_weight), sends)
        ]

    def send_own(target):
        for copy in pair(boxes_ref, own_weight, col, target, (box_send, weight_send)):
            copy.start()

    def send_chip(target):
        send_own(target * 2 + jnp.where(before_late & (target == n_chip - 1), 0, 1))

    along(before, send_chip)
    along(after, send_chip)
    send_own(partner)

    pl.when(chip == n_chip - 1)(suffix_sums)

    def below_copy(bit):
        return pltpu.make_async_remote_copy(
            src_ref=below_out.at[bit], dst_ref=below_in.at[bit], send_sem=below_send,
            recv_sem=below_recv.at[bit], device_id=(flipped(flips[bit]), col), device_id_type=MESH,
        )

    below_copy(0).start()

    @pl.when(waits_far)
    def _():
        pl.semaphore_wait(far_in, 1)
        pl.when(core == 1)(lambda: tell_far(partner))
        along(beyond, send_chip)
        pl.when((core == 1) & tells_far)(tell_below)

    def take_below(bit):
        below_copy(bit).wait_recv()
        if bit + 1 < len(flips):
            below_out[bit + 1] = below_out[bit] + below_in[bit]
            below_copy(bit + 1).start()

    row_start = row * rows
    col_start = col * cols
    one8, zero8 = jnp.ones((rows, block), F8), jnp.zeros((rows, block), F8)
    low_end = jnp.int16(-32768)

    def raster(slot):
        ys, xs = iota(rows) + low_end, iota(cols) + low_end
        for index in range(nets // block):
            at = pl.ds(index * block, block)
            unit, stage = index % 2, index // 2 % 2
            x0, x1 = held_box[slot, 0:1, at], held_box[slot, 1:2, at]
            y0, y1 = held_box[slot, 2:3, at], held_box[slot, 3:4, at]
            scaled = held_weight[slot, :, at] * 16.0
            high = scaled.astype(F8)
            low = ((scaled - high.astype(F32)) * 16.0).astype(F8)
            down = ys - (y0 - row_start).astype(I16) <= (y1 - y0 - 32768).astype(I16)
            across = xs - (x0 - col_start).astype(I16) <= (x1 - x0 - 32768).astype(I16)
            weighted = jnp.concatenate(
                [jnp.where(across, jnp.broadcast_to(part, (cols, block)), zero8[:cols]) for part in (high, low)], axis=0
            )
            pltpu.matmul_push_rhs(weighted, staging_register=stage, mxu_index=unit, transpose=True)
            pltpu.matmul_acc_lhs(sums[unit], jnp.where(down, one8, zero8), load_staged_rhs=stage)

    def wait_pair(slot):
        pltpu.make_async_remote_copy(
            src_ref=net_rows, dst_ref=net_rows, send_sem=box_send, recv_sem=net_recv.at[slot],
            device_id=(row, partner), device_id_type=MESH,
        ).wait_recv()


    far_rows = [mask for mask in range(1, n_row) if mask not in flips]

    def scan_rows():
        for bit in range(len(flips) - 1):
            take_below(bit)

    def tell_rows():
        for mask in far_rows:
            pl.semaphore_signal(token, inc=1, device_id=(flipped(mask), col), device_id_type=MESH)

    def take(slot, ready, then=lambda: None):
        direct = late & (slot == n_col - 4)
        hub = (core == 1) & jnp.logical_not(direct)

        def pass_on():
            for copy in pair(held_box.at[slot], held_weight.at[slot], slot, partner, (pass_box, pass_weight)):
                copy.start()

        @pl.when(hub)
        def _():
            wait_pair(slot)
            pass_on()
            then()

        raster(ready)

        @pl.when(jnp.logical_not(hub))
        def _():
            wait_pair(slot)
            pl.when((core == 0) & direct)(pass_on)

    raster(col)
    wait_pair(partner)
    ready = partner
    pl.when(jnp.logical_not(late))(scan_rows)
    if n_chip == len(ORDER):
        for step in range(n_col - 2):
            slot = sum(jnp.where(chip == at, ORDER[at][step], 0) for at in range(n_chip))
            slot = jnp.where(late & (core == 0), LATE[step], slot)
            known = sum(jnp.where(chip == at, KNOWN[at] == step, False) for at in range(n_chip)) > 0
            take(slot, ready, (lambda: pl.when(known)(tell_rows)) if step in KNOWN else lambda: None)
            ready = slot
            if step == 1:
                pl.when(late)(scan_rows)
    else:
        for side in (1, 0):
            def step(index, ready):
                slot = nearest(index) * 2 + side
                take(slot, ready)
                return slot

            ready = lax.fori_loop(1, n_chip, step, ready)
            if side:
                pl.when(late)(scan_rows)
                pl.when(core == 1)(tell_rows)
    raster(ready)
    take_below(len(flips) - 1)
    below = jnp.zeros((1, cols), F32)
    for bit, flip in enumerate(flips):
        below += jnp.where(row // flip % 2 == 0, below_in[bit], jnp.zeros((), F32))

    @pl.when(core == 1)
    def _():
        pl.semaphore_wait(token, len(far_rows))
        pl.semaphore_signal(token, inc=1, device_id=(row, partner), device_id_type=MESH)

    @pl.when(core == 0)
    def _():
        pl.semaphore_wait(token, 1)

    landed(2, cap_ref)
    both = pltpu.matmul_pop(sums[0]) + pltpu.matmul_pop(sums[1])
    acc[...] = both[:, :cols] * (1.0 / 16.0) + both[:, cols:] * (1.0 / 256.0)
    excess = jnp.maximum(acc[...] - cap_ref[...], 0.0)
    col_out[...] = jnp.sum(excess, axis=0, keepdims=True)
    growth = jnp.sum(excess * (suffix[...] + below), axis=0, keepdims=True)
    msg[me, 0:1, :] = growth

    def column_copy(offset):
        target = lax.rem(row + offset, n_row)
        return pltpu.make_async_remote_copy(
            src_ref=col_out, dst_ref=col_in.at[row], send_sem=col_send, recv_sem=col_recv,
            device_id=(target, col), device_id_type=MESH,
        )

    for offset in range(1, n_row):
        column_copy(offset).start()

    def message(mask, step, side):
        target = (nearest(step) if step else chip) * 2 + (core if side else 1 - core)
        return pltpu.make_async_remote_copy(
            src_ref=msg.at[me], dst_ref=msg.at[me], send_sem=msg_send, recv_sem=msg_recv,
            device_id=(flipped(mask), target), device_id_type=MESH,
        )

    def hops(at):
        mask, step, _ = at
        return -(mask.bit_count() + step)

    everyone = [(mask, step, side) for mask in range(n_row) for step in range(n_chip) for side in (0, 1)]
    for at in sorted(everyone, key=hops):
        if at != (0, 0, 1):
            message(*at).start()

    parts = jnp.concatenate(split2(excess), axis=1)
    for index in range(rows // block):
        unit, stage = index % 2, index // 2 % 2
        above = lax.broadcasted_iota(jnp.int32, (rows, block), 1).astype(I16) + jnp.int16(index * block)
        lower = jnp.where(iota(rows) >= above, one, zero)
        pltpu.matmul_push_rhs(parts[index * block:(index + 1) * block], staging_register=stage, mxu_index=unit)
        pltpu.matmul_acc_lhs(sums[unit], lower, load_staged_rhs=stage)
    both = pltpu.matmul_pop(sums[0]) + pltpu.matmul_pop(sums[1])
    within = both[:, :cols] + both[:, cols:]
    within_ref[...] = within
    table[...] = jnp.concatenate(split2(within.T), axis=0)
    columns = lax.broadcasted_iota(jnp.int32, (cols, block), 0)
    for index in range(cells // block):
        bin_row, bin_col, _ = cell_block(index, block)
        unit = index % 2
        got = looks[index % len(looks)]
        for part in range(rows // block):
            at = pl.ds(part * block, block)
            same = jnp.where(iota(block) == (bin_row - part * block).astype(I16), one, zero)
            pltpu.matmul_push_rhs(same, staging_register=part % 2, mxu_index=unit)
            pltpu.matmul_acc_lhs(got, table[:, at], load_staged_rhs=part % 2)
        got = pltpu.matmul_pop(got)
        got = jnp.where(columns == bin_col, got[:cols] + got[cols:], 0.0)
        looked[:, pl.ds(index * block, block)] = jnp.sum(got, axis=0, keepdims=True)

    def drain(like, send, recv=None):
        copy = pltpu.make_async_remote_copy(
            src_ref=like, dst_ref=like, send_sem=send, recv_sem=col_recv if recv is None else recv,
            device_id=(row, partner), device_id_type=MESH,
        )
        copy.wait_send()
        if recv is not None:
            copy.wait_recv()

    drain(held_box.at[pl.ds(0, n_chip)], box_send)
    drain(held_weight.at[pl.ds(0, n_chip)], weight_send)

    def passed(units):
        drain(held_box.at[pl.ds(0, units)], pass_box)
        drain(held_weight.at[pl.ds(0, units)], pass_weight)

    for units, who in (
        (n_col - 2, (core == 1) & jnp.logical_not(late)), (n_col - 3, (core == 1) & late), (1, (core == 0) & late)
    ):
        pl.when(who)(functools.partial(passed, units))

    drain(below_out.at[pl.ds(0, len(flips))], below_send)
    drain(col_in.at[pl.ds(0, n_row - 1)], col_send, col_recv)
    carried = jnp.zeros((1, cols), F32)
    for index in range(n_row):
        carried += jnp.where(index < row, col_in[index], jnp.zeros((), F32))
    scale = 2.0 / (rows * n_row)
    turned_carry = jnp.broadcast_to(carried, (8, cols)).T[:, 0:1]
    for index in range(cells // block):
        at = pl.ds(index * block, block)
        _, bin_col, area = cell_block(index, block)
        got = jnp.where(columns == bin_col, turned_carry, 0.0)
        got = looked[:, at] + jnp.sum(got, axis=0, keepdims=True)
        looked[:, at] = area * (1.0 + scale * got)
    final_ref[...] = jnp.broadcast_to(1.0 + scale * carried, final_ref.shape)

    drain(msg.at[pl.ds(0, n_row * n_col - 1)], msg_send, msg_recv)
    rows_left = [msg[index] for index in range(n_row * n_col)]
    while len(rows_left) > 1:
        rows_left = [sum(rows_left[at:at + 2]) for at in range(0, len(rows_left), 2)]
    totals = jnp.broadcast_to(jnp.sum(rows_left[0], axis=1, keepdims=True), (2, cols))
    area_total = totals[1:2]
    ratio = area_total / (area_total + scale * totals[0:1])
    for index in range(cells // cols):
        at = pl.ds(index * cols, cols)
        size_ref[:, at] = looked[:, at] * ratio


def with_units(body, *refs):
    rows, cols = refs[5].shape
    wide = 2 * cols
    pl.run_scoped(
        functools.partial(body, *refs),
        *[pltpu.ACC(unit)((rows, wide), F32) for unit in (0, 1)],
        *[pltpu.ACC(unit)((wide, wide), F32) for unit in (0, 1, 0, 1)],
    )


def finish(scale, rudy, within, size, final, rudy_hbm, infl_hbm, size_hbm, infl, sems):
    first = pltpu.make_async_copy(rudy, rudy_hbm, sems.at[0])
    second = pltpu.make_async_copy(size, size_hbm, sems.at[1])
    third = pltpu.make_async_copy(infl, infl_hbm, sems.at[2])
    first.start()
    second.start()
    infl[...] = final[0:1, :] + scale * within[...]
    third.start()
    first.wait()
    second.wait()
    third.wait()


def solution(mesh):
    n_row, n_col = mesh.shape["row"], mesh.shape["col"]

    def per_device(boxes, pins, capacity, cell_bin, cell_area):
        rows, cols = capacity.shape
        nets = boxes.shape[1]
        cells = cell_bin.shape[1]
        vmem = pl.BlockSpec(memory_space=pltpu.VMEM)
        hbm = pl.BlockSpec(memory_space=pl.ANY)
        dma = pltpu.SemaphoreType.DMA
        rudy, within, size, final = pl.pallas_call(
            functools.partial(with_units, functools.partial(kernel, n_row, n_col)),
            out_shape=(
                pltpu.VMEM((rows, cols), F32),
                pltpu.VMEM((rows, cols), F32),
                pltpu.VMEM((1, cells), F32),
                pltpu.VMEM((8, cols), F32),
            ),
            in_specs=[hbm] * 5,
            out_specs=(vmem,) * 4,
            scratch_shapes=[
                pltpu.VMEM((4, nets), jnp.int32),
                pltpu.VMEM((1, nets), jnp.int32),
                pltpu.VMEM((rows, cols), F32),
                pltpu.VMEM((1, cells), jnp.int32),
                pltpu.VMEM((1, cells), F32),
                pltpu.VMEM((n_col, 4, nets), jnp.int32),
                pltpu.VMEM((n_col, 1, nets), F32),
                pltpu.VMEM((1, nets), F32),
                pltpu.VMEM((rows, cols), F32),
                pltpu.VMEM((n_row, 1, cols), F32),
                pltpu.VMEM((n_row, 1, cols), F32),
                pltpu.VMEM((n_row * n_col, 2, cols), F32),
                pltpu.VMEM((1, cols), F32),
                pltpu.VMEM((n_row, 1, cols), F32),
                pltpu.VMEM((1, cells), F32),
                dma, dma, dma, dma, dma((n_col,)), pltpu.SemaphoreType.REGULAR, pltpu.SemaphoreType.REGULAR,
                dma, dma((n_row.bit_length() - 1,)), dma, dma, dma, dma, dma((3,)),
                pltpu.VMEM((2 * cols, rows), BF16),
            ],
            compiler_params=pltpu.CompilerParams(
                collective_id=0, has_side_effects=True,
            ),
        )(boxes, pins[None, :], capacity, cell_bin, cell_area)
        return pl.pallas_call(
            functools.partial(finish, 2.0 / (rows * n_row)),
            out_shape=(
                jax.ShapeDtypeStruct((rows, cols), F32),
                jax.ShapeDtypeStruct((rows, cols), F32),
                jax.ShapeDtypeStruct((1, cells), F32),
            ),
            in_specs=[vmem] * 4,
            out_specs=(hbm,) * 3,
            scratch_shapes=[pltpu.VMEM((rows, cols), F32), dma((3,))],
        )(*[pltpu.with_memory_space_constraint(value, pltpu.VMEM) for value in (rudy, within, size, final)])

    in_specs = (P(None, "col"), P("col"), P("row", "col"), P("row", "col"), P("row", "col"))
    out_specs = (P("row", "col"), P("row", "col"), P("row", "col"))
    return jax.shard_map(
        per_device, mesh=mesh, in_specs=in_specs, out_specs=out_specs, check_vma=False
    )
```

```python
import functools

import jax
import jax.numpy as jnp
from jax import lax
from jax.experimental import pallas as pl
from jax.experimental.pallas import tpu as pltpu
from jax.sharding import PartitionSpec as P

MESH = pl.DeviceIdType.MESH
F32 = jnp.float32
I16 = jnp.int16
F8 = jnp.float8_e4m3fn
BF16 = jnp.bfloat16
NT = (((1,), (1,)), ((), ()))
NN = (((1,), (0,)), ((), ()))


ORDER = ((3, 5, 7, 2, 6, 4), (1, 7, 0, 6, 5, 4), (1, 7, 0, 6, 3, 2), (5, 3, 2, 1, 0, 4))
LATE = (5, 4, 3, 2, 1, 0)
KNOWN = tuple(max(at for at, slot in enumerate(order) if slot % 2) for order in ORDER)


def split2(value):
    high = value.astype(BF16)
    return high, (value - high.astype(F32)).astype(BF16)


def kernel(
    n_row, n_col,
    boxes_hbm, pins_hbm, cap_hbm, bin_hbm, area_hbm,
    acc, within_ref, size_ref, final_ref,
    boxes_ref, pins_ref, cap_ref, bin_ref, area_ref,
    held_box, held_weight, own_weight, suffix, below_out, below_in, msg, col_out, col_in, looked,
    box_send, weight_send, pass_box, pass_weight, net_recv, token, far_in,
    below_send, below_recv, col_send, col_recv, msg_send, msg_recv, load_sem, table, *units,
):
    sums, looks = units[:2], units[2:]
    rows, cols = acc.shape
    nets = boxes_ref.shape[1]
    cells = bin_ref.shape[1]
    n_chip = n_col // 2
    row = lax.axis_index("row")
    col = lax.axis_index("col")
    chip, core = col // 2, col % 2
    partner = chip * 2 + (1 - core)
    me = row * n_col + col

    both_sides = jnp.minimum(chip, n_chip - 1 - chip)
    longer = jnp.where(chip < n_chip - 1 - chip, 1, -1)

    def nearest(step):
        turn = jnp.where(lax.rem(step, 2) == 1, 1, -1) * ((step + 1) // 2)
        return chip + jnp.where(step <= 2 * both_sides, turn, longer * (step - both_sides))

    reach = min(2, n_chip - 1)
    flips = [1 << bit for bit in range(n_row.bit_length() - 1)]

    def flipped(mask):
        other = row
        for flip in flips:
            if mask & flip:
                other = other + flip * (1 - 2 * (row // flip % 2))
        return other

    sources = [(boxes_hbm, boxes_ref, 0), (pins_hbm, pins_ref, 0), (bin_hbm, bin_ref, 1), (area_hbm, area_ref, 1)]
    for source, target, index in (*sources, (cap_hbm, cap_ref, 2)):
        pltpu.make_async_copy(source, target, load_sem.at[index]).start()

    def along(offsets, act):
        for offset in offsets:
            target = chip + offset

            @pl.when((target >= 0) & (target < n_chip))
            def _():
                act(target)

    before = range(1 - n_chip, 0)
    after = range(reach, 0, -1)
    beyond = range(n_chip - 1, reach, -1)
    late = chip == n_chip - 1
    before_late = (core == 0) & (chip == n_chip - 2)
    relayed = n_chip == len(ORDER)
    spares = (core == 1) & (chip == n_chip - 4) & relayed
    relays = (core == 1) & (chip == n_chip - 2) & relayed
    waits_far = chip < n_chip - 1 - reach
    tells_far = (chip > 0) & (chip < n_chip - reach)

    barrier = pltpu.get_barrier_semaphore()

    def greet(target_row, target_col):
        pl.semaphore_signal(barrier, inc=1, device_id=(target_row, target_col), device_id_type=MESH)

    @pl.when(core == 1)
    def _():
        for side in (1, 0):
            along([-offset for offset in (*after, *before)], lambda target: greet(row, target * 2 + side))

    @pl.when((core == 0) & late)
    def _():
        greet(row, col - 2)

    greet(row, partner)
    for flip in flips:
        greet(flipped(flip), col)

    def tell_far(target):
        pl.semaphore_signal(far_in, inc=1, device_id=(row, target), device_id_type=MESH)

    def tell_below():
        tell_far(jnp.maximum(chip - 1, 0) * 2 + 1)

    def landed(index, like):
        pltpu.make_async_copy(like, like, load_sem.at[index]).wait()

    net_rows = acc.at[pl.ds(0, 5 * nets // cols)]
    for unit in (*sums, *looks):
        pltpu.matmul_pop(unit)
    landed(0, net_rows)

    span_x = (boxes_ref[1:2, :] - boxes_ref[0:1, :] + 1).astype(F32)
    span_y = (boxes_ref[3:4, :] - boxes_ref[2:3, :] + 1).astype(F32)
    weight = jnp.log(pins_ref[...].astype(F32)) * (span_x + span_y) / (span_x * span_y)
    weight = weight.astype(BF16).astype(F32)
    own_weight[...] = weight
    held_weight[col] = weight
    held_box[col] = boxes_ref[...]

    landed(1, held_weight.at[pl.ds(0, 2)])

    def cell_block(index, size):
        at = pl.ds(index * size, size)
        value = bin_ref[:, at]
        return lax.shift_right_logical(value, cols.bit_length() - 1), value & (cols - 1), area_ref[:, at]

    block = 256
    one, zero = jnp.ones((), BF16), jnp.zeros((), BF16)

    def iota(length, width=block):
        return lax.broadcasted_iota(jnp.int32, (length, width), 0).astype(I16)

    def suffix_sums():
        for index in range(cells // block):
            bin_row, bin_col, area = cell_block(index, block)
            unit, stage = index % 2, index // 2 % 2
            at_or_below = jnp.where(iota(rows) <= bin_row.astype(I16), one, zero)
            high, low = split2(area)
            same = iota(cols) == bin_col.astype(I16)
            held = jnp.concatenate([jnp.where(same, high, zero), jnp.where(same, low, zero)], axis=0)
            pltpu.matmul_push_rhs(held, staging_register=stage, mxu_index=unit, transpose=True)
            pltpu.matmul_acc_lhs(sums[unit], at_or_below, load_staged_rhs=stage)
        total = pltpu.matmul_pop(sums[0]) + pltpu.matmul_pop(sums[1])
        suffix[...] = total[:, :cols] + total[:, cols:]
        below_out[0] = suffix[0:1, :]
        msg[me, 1:2, :] = suffix[0:1, :]

    pl.when(chip < n_chip - 1)(suffix_sums)

    around = chip + jnp.minimum(n_chip - 1 - chip, reach)
    pl.semaphore_wait(barrier, around + 1 + len(flips) + jnp.where(before_late, 1, 0))
    pl.when((core == 1) & tells_far & jnp.logical_not(waits_far))(tell_below)

    def pair(source, weight_source, slot, target, sends):
        return [
            pltpu.make_async_remote_copy(
                src_ref=src, dst_ref=held.at[slot], send_sem=send, recv_sem=net_recv.at[slot],
                device_id=(row, target), device_id_type=MESH,
            )
            for src, held, send in zip((source, weight_source), (held_box, held_weight), sends)
        ]

    def send_own(target):
        for copy in pair(boxes_ref, own_weight, col, target, (box_send, weight_send)):
            copy.start()

    def send_chip(target):
        @pl.when(jnp.logical_not(spares & (target == n_chip - 1)))
        def _():
            send_own(target * 2 + jnp.where(before_late & (target == n_chip - 1), 0, 1))

    along(before, send_chip)
    along(after, send_chip)
    send_own(partner)

    pl.when(chip == n_chip - 1)(suffix_sums)

    def below_copy(bit):
        return pltpu.make_async_remote_copy(
            src_ref=below_out.at[bit], dst_ref=below_in.at[bit], send_sem=below_send,
            recv_sem=below_recv.at[bit], device_id=(flipped(flips[bit]), col), device_id_type=MESH,
        )

    below_copy(0).start()

    @pl.when(waits_far)
    def _():
        pl.semaphore_wait(far_in, 1)
        pl.when(core == 1)(lambda: tell_far(partner))
        along(beyond, send_chip)
        pl.when((core == 1) & tells_far)(tell_below)

    def take_below(bit):
        below_copy(bit).wait_recv()
        if bit + 1 < len(flips):
            below_out[bit + 1] = below_out[bit] + below_in[bit]
            below_copy(bit + 1).start()

    row_start = row * rows
    col_start = col * cols
    one8, zero8 = jnp.ones((rows, block), F8), jnp.zeros((rows, block), F8)
    low_end = jnp.int16(-32768)

    def raster(slot):
        ys, xs = iota(rows) + low_end, iota(cols) + low_end
        for index in range(nets // block):
            at = pl.ds(index * block, block)
            unit, stage = index % 2, index // 2 % 2
            x0, x1 = held_box[slot, 0:1, at], held_box[slot, 1:2, at]
            y0, y1 = held_box[slot, 2:3, at], held_box[slot, 3:4, at]
            scaled = held_weight[slot, :, at] * 16.0
            high = scaled.astype(F8)
            low = ((scaled - high.astype(F32)) * 16.0).astype(F8)
            down = ys - (y0 - row_start).astype(I16) <= (y1 - y0 - 32768).astype(I16)
            across = xs - (x0 - col_start).astype(I16) <= (x1 - x0 - 32768).astype(I16)
            weighted = jnp.concatenate(
                [jnp.where(across, jnp.broadcast_to(part, (cols, block)), zero8[:cols]) for part in (high, low)], axis=0
            )
            pltpu.matmul_push_rhs(weighted, staging_register=stage, mxu_index=unit, transpose=True)
            pltpu.matmul_acc_lhs(sums[unit], jnp.where(down, one8, zero8), load_staged_rhs=stage)

    def wait_pair(slot):
        pltpu.make_async_remote_copy(
            src_ref=net_rows, dst_ref=net_rows, send_sem=box_send, recv_sem=net_recv.at[slot],
            device_id=(row, partner), device_id_type=MESH,
        ).wait_recv()


    far_rows = [mask for mask in range(1, n_row) if mask not in flips]

    def scan_rows():
        for bit in range(len(flips) - 1):
            take_below(bit)

    def tell_rows():
        for mask in far_rows:
            pl.semaphore_signal(token, inc=1, device_id=(flipped(mask), col), device_id_type=MESH)

    def take(slot, ready, then=lambda: None):
        direct = late & (slot == n_col - 4)
        hub = (core == 1) & jnp.logical_not(direct)

        def pass_on():
            for copy in pair(held_box.at[slot], held_weight.at[slot], slot, partner, (pass_box, pass_weight)):
                copy.start()

        @pl.when(hub)
        def _():
            wait_pair(slot)

            @pl.when(relays & (slot == n_col - 7))
            def _():
                for copy in pair(held_box.at[slot], held_weight.at[slot], slot, n_col - 1, (pass_box, pass_weight)):
                    copy.start()

            pass_on()
            then()

        raster(ready)

        @pl.when(jnp.logical_not(hub))
        def _():
            wait_pair(slot)
            pl.when((core == 0) & direct)(pass_on)

    raster(col)
    wait_pair(partner)
    ready = partner
    pl.when(jnp.logical_not(late))(scan_rows)
    if n_chip == len(ORDER):
        for step in range(n_col - 2):
            slot = sum(jnp.where(chip == at, ORDER[at][step], 0) for at in range(n_chip))
            slot = jnp.where(late & (core == 0), LATE[step], slot)
            known = sum(jnp.where(chip == at, KNOWN[at] == step, False) for at in range(n_chip)) > 0
            take(slot, ready, (lambda: pl.when(known)(tell_rows)) if step in KNOWN else lambda: None)
            ready = slot
            if step == 1:
                pl.when(late)(scan_rows)
    else:
        for side in (1, 0):
            def step(index, ready):
                slot = nearest(index) * 2 + side
                take(slot, ready)
                return slot

            ready = lax.fori_loop(1, n_chip, step, ready)
            if side:
                pl.when(late)(scan_rows)
                pl.when(core == 1)(tell_rows)
    raster(ready)
    take_below(len(flips) - 1)
    below = jnp.zeros((1, cols), F32)
    for bit, flip in enumerate(flips):
        below += jnp.where(row // flip % 2 == 0, below_in[bit], jnp.zeros((), F32))

    @pl.when(core == 1)
    def _():
        pl.semaphore_wait(token, len(far_rows))
        pl.semaphore_signal(token, inc=1, device_id=(row, partner), device_id_type=MESH)

    @pl.when(core == 0)
    def _():
        pl.semaphore_wait(token, 1)

    landed(2, cap_ref)
    both = pltpu.matmul_pop(sums[0]) + pltpu.matmul_pop(sums[1])
    acc[...] = both[:, :cols] * (1.0 / 16.0) + both[:, cols:] * (1.0 / 256.0)
    excess = jnp.maximum(acc[...] - cap_ref[...], 0.0)
    col_out[...] = jnp.sum(excess, axis=0, keepdims=True)
    growth = jnp.sum(excess * (suffix[...] + below), axis=0, keepdims=True)
    msg[me, 0:1, :] = growth

    def column_copy(offset):
        target = lax.rem(row + offset, n_row)
        return pltpu.make_async_remote_copy(
            src_ref=col_out, dst_ref=col_in.at[row], send_sem=col_send, recv_sem=col_recv,
            device_id=(target, col), device_id_type=MESH,
        )

    for offset in range(1, n_row):
        column_copy(offset).start()

    def message(mask, step, side):
        target = (nearest(step) if step else chip) * 2 + (core if side else 1 - core)
        return pltpu.make_async_remote_copy(
            src_ref=msg.at[me], dst_ref=msg.at[me], send_sem=msg_send, recv_sem=msg_recv,
            device_id=(flipped(mask), target), device_id_type=MESH,
        )

    def hops(at):
        mask, step, _ = at
        return -(mask.bit_count() + step)

    everyone = [(mask, step, side) for mask in range(n_row) for step in range(n_chip) for side in (0, 1)]
    for at in sorted(everyone, key=hops):
        if at != (0, 0, 1):
            message(*at).start()

    parts = jnp.concatenate(split2(excess), axis=1)
    for index in range(rows // block):
        unit, stage = index % 2, index // 2 % 2
        above = lax.broadcasted_iota(jnp.int32, (rows, block), 1).astype(I16) + jnp.int16(index * block)
        lower = jnp.where(iota(rows) >= above, one, zero)
        pltpu.matmul_push_rhs(parts[index * block:(index + 1) * block], staging_register=stage, mxu_index=unit)
        pltpu.matmul_acc_lhs(sums[unit], lower, load_staged_rhs=stage)
    both = pltpu.matmul_pop(sums[0]) + pltpu.matmul_pop(sums[1])
    within = both[:, :cols] + both[:, cols:]
    within_ref[...] = within
    table[...] = jnp.concatenate(split2(within.T), axis=0)
    columns = lax.broadcasted_iota(jnp.int32, (cols, block), 0)
    for index in range(cells // block):
        bin_row, bin_col, _ = cell_block(index, block)
        unit = index % 2
        got = looks[index % len(looks)]
        for part in range(rows // block):
            at = pl.ds(part * block, block)
            same = jnp.where(iota(block) == (bin_row - part * block).astype(I16), one, zero)
            pltpu.matmul_push_rhs(same, staging_register=part % 2, mxu_index=unit)
            pltpu.matmul_acc_lhs(got, table[:, at], load_staged_rhs=part % 2)
        got = pltpu.matmul_pop(got)
        got = jnp.where(columns == bin_col, got[:cols] + got[cols:], 0.0)
        looked[:, pl.ds(index * block, block)] = jnp.sum(got, axis=0, keepdims=True)

    def drain(like, send, recv=None):
        copy = pltpu.make_async_remote_copy(
            src_ref=like, dst_ref=like, send_sem=send, recv_sem=col_recv if recv is None else recv,
            device_id=(row, partner), device_id_type=MESH,
        )
        copy.wait_send()
        if recv is not None:
            copy.wait_recv()

    def own_sent(units):
        drain(held_box.at[pl.ds(0, units)], box_send)
        drain(held_weight.at[pl.ds(0, units)], weight_send)

    pl.when(spares)(lambda: own_sent(n_chip - 1))
    pl.when(jnp.logical_not(spares))(lambda: own_sent(n_chip))

    def passed(units):
        drain(held_box.at[pl.ds(0, units)], pass_box)
        drain(held_weight.at[pl.ds(0, units)], pass_weight)

    for units, who in (
        (n_col - 1, relays), (n_col - 2, (core == 1) & jnp.logical_not(late | relays)), (n_col - 3, (core == 1) & late), (1, (core == 0) & late)
    ):
        pl.when(who)(functools.partial(passed, units))

    drain(below_out.at[pl.ds(0, len(flips))], below_send)
    drain(col_in.at[pl.ds(0, n_row - 1)], col_send, col_recv)
    carried = jnp.zeros((1, cols), F32)
    for index in range(n_row):
        carried += jnp.where(index < row, col_in[index], jnp.zeros((), F32))
    scale = 2.0 / (rows * n_row)
    turned_carry = jnp.broadcast_to(carried, (8, cols)).T[:, 0:1]
    for index in range(cells // block):
        at = pl.ds(index * block, block)
        _, bin_col, area = cell_block(index, block)
        got = jnp.where(columns == bin_col, turned_carry, 0.0)
        got = looked[:, at] + jnp.sum(got, axis=0, keepdims=True)
        looked[:, at] = area * (1.0 + scale * got)
    final_ref[...] = jnp.broadcast_to(1.0 + scale * carried, final_ref.shape)

    drain(msg.at[pl.ds(0, n_row * n_col - 1)], msg_send, msg_recv)
    rows_left = [msg[index] for index in range(n_row * n_col)]
    while len(rows_left) > 1:
        rows_left = [sum(rows_left[at:at + 2]) for at in range(0, len(rows_left), 2)]
    totals = jnp.broadcast_to(jnp.sum(rows_left[0], axis=1, keepdims=True), (2, cols))
    area_total = totals[1:2]
    ratio = area_total / (area_total + scale * totals[0:1])
    for index in range(cells // cols):
        at = pl.ds(index * cols, cols)
        size_ref[:, at] = looked[:, at] * ratio


def with_units(body, *refs):
    rows, cols = refs[5].shape
    wide = 2 * cols
    pl.run_scoped(
        functools.partial(body, *refs),
        *[pltpu.ACC(unit)((rows, wide), F32) for unit in (0, 1)],
        *[pltpu.ACC(unit)((wide, wide), F32) for unit in (0, 1, 0, 1)],
    )


def finish(scale, rudy, within, size, final, rudy_hbm, infl_hbm, size_hbm, infl, sems):
    first = pltpu.make_async_copy(rudy, rudy_hbm, sems.at[0])
    second = pltpu.make_async_copy(size, size_hbm, sems.at[1])
    third = pltpu.make_async_copy(infl, infl_hbm, sems.at[2])
    first.start()
    second.start()
    infl[...] = final[0:1, :] + scale * within[...]
    third.start()
    first.wait()
    second.wait()
    third.wait()


def solution(mesh):
    n_row, n_col = mesh.shape["row"], mesh.shape["col"]

    def per_device(boxes, pins, capacity, cell_bin, cell_area):
        rows, cols = capacity.shape
        nets = boxes.shape[1]
        cells = cell_bin.shape[1]
        vmem = pl.BlockSpec(memory_space=pltpu.VMEM)
        hbm = pl.BlockSpec(memory_space=pl.ANY)
        dma = pltpu.SemaphoreType.DMA
        rudy, within, size, final = pl.pallas_call(
            functools.partial(with_units, functools.partial(kernel, n_row, n_col)),
            out_shape=(
                pltpu.VMEM((rows, cols), F32),
                pltpu.VMEM((rows, cols), F32),
                pltpu.VMEM((1, cells), F32),
                pltpu.VMEM((8, cols), F32),
            ),
            in_specs=[hbm] * 5,
            out_specs=(vmem,) * 4,
            scratch_shapes=[
                pltpu.VMEM((4, nets), jnp.int32),
                pltpu.VMEM((1, nets), jnp.int32),
                pltpu.VMEM((rows, cols), F32),
                pltpu.VMEM((1, cells), jnp.int32),
                pltpu.VMEM((1, cells), F32),
                pltpu.VMEM((n_col, 4, nets), jnp.int32),
                pltpu.VMEM((n_col, 1, nets), F32),
                pltpu.VMEM((1, nets), F32),
                pltpu.VMEM((rows, cols), F32),
                pltpu.VMEM((n_row, 1, cols), F32),
                pltpu.VMEM((n_row, 1, cols), F32),
                pltpu.VMEM((n_row * n_col, 2, cols), F32),
                pltpu.VMEM((1, cols), F32),
                pltpu.VMEM((n_row, 1, cols), F32),
                pltpu.VMEM((1, cells), F32),
                dma, dma, dma, dma, dma((n_col,)), pltpu.SemaphoreType.REGULAR, pltpu.SemaphoreType.REGULAR,
                dma, dma((n_row.bit_length() - 1,)), dma, dma, dma, dma, dma((3,)),
                pltpu.VMEM((2 * cols, rows), BF16),
            ],
            compiler_params=pltpu.CompilerParams(
                collective_id=0, has_side_effects=True,
            ),
        )(boxes, pins[None, :], capacity, cell_bin, cell_area)
        return pl.pallas_call(
            functools.partial(finish, 2.0 / (rows * n_row)),
            out_shape=(
                jax.ShapeDtypeStruct((rows, cols), F32),
                jax.ShapeDtypeStruct((rows, cols), F32),
                jax.ShapeDtypeStruct((1, cells), F32),
            ),
            in_specs=[vmem] * 4,
            out_specs=(hbm,) * 3,
            scratch_shapes=[pltpu.VMEM((rows, cols), F32), dma((3,))],
        )(*[pltpu.with_memory_space_constraint(value, pltpu.VMEM) for value in (rudy, within, size, final)])

    in_specs = (P(None, "col"), P("col"), P("row", "col"), P("row", "col"), P("row", "col"))
    out_specs = (P("row", "col"), P("row", "col"), P("row", "col"))
    return jax.shard_map(
        per_device, mesh=mesh, in_specs=in_specs, out_specs=out_specs, check_vma=False
    )
```
